32 devices in a mesh: ga: 16 (over z, y, x), band: 2 (over core).
Axes of the slice: x: 2, y: 2, z: 4, core: 2. Of those that a mesh axis runs over, the one named last changes fastest.
Arguments:
- coefficients: float32 [2048, 2, 8192], P('band', None, 'ga'), may hold values from -6 to 6
- rotation: float32 [2, 2048, 32], P(None, 'band', 'ga'), may hold values from -0.125 to 0.125
- potential: float32 [64, 4096], P(None, 'ga'), may hold values from -2 to 0.5
- index_map: int32 [8192], replicated, may hold values from 0 to 262143, as said below
- counts: int32 [16], replicated, may hold values from 384 to 512, as said below
Outputs:
- applied_panel: float32 [32, 2, 32, 1024], P(('band', 'ga'))
The draws below stay inside these ranges and needn't reach their ends.
Inputs may be any that keep to these rules, and one draw needn't show every extreme that they name: counts[i] counts the live slots of index i of ga, which are its slots 0 to counts[i] - 1 of 512; the counts sum to 7168, and some index has exactly 512. `index_map`: live slots name distinct cells, and together exactly 7168 cells whose signed frequency vector has a squared length no larger than that of any cell not named (a ball about the anchor), every signed component of a live cell lying in -16 to 15; dead slots name arbitrary cells.
All inputs are finite; a program needn't handle non-finite values.
Results may differ from the reference program's by a relative error of at most 0.00008.
Values sent between devices are 32-bit elements; how exact they have to be, the bound alone decides.
A program may use at most 128 MiB of HBM per device.

```python
import jax
import jax.numpy as jnp
from jax import lax

BANDS = 2048
BOX = 64
SLOT_DEV = 512
PW_DEV = 448
NPW = 7168
PANEL = 32
N_GA = 16


def layout_draw(key):
    folded = jax.random.fold_in(key, 7)
    key_ties, key_shuffle, key_pairs, key_order, key_dead = jax.random.split(folded, 5)
    cell_count = BOX * BOX * BOX
    flat_cells = jnp.arange(cell_count, dtype=jnp.int32)
    freq_x = flat_cells // (BOX * BOX)
    freq_y = flat_cells // BOX % BOX
    freq_z = flat_cells % BOX
    freq_x = jnp.where(freq_x >= BOX // 2, freq_x - BOX, freq_x)
    freq_y = jnp.where(freq_y >= BOX // 2, freq_y - BOX, freq_y)
    freq_z = jnp.where(freq_z >= BOX // 2, freq_z - BOX, freq_z)
    squared_norm = freq_x * freq_x + freq_y * freq_y + freq_z * freq_z
    ties_rank = jax.random.permutation(key_ties, cell_count).astype(jnp.int32)
    ranking = jnp.argsort(squared_norm * cell_count + ties_rank, stable=True).astype(jnp.int32)
    ball_cells = jax.random.permutation(key_shuffle, ranking[:NPW])
    dead_mean = SLOT_DEV - PW_DEV
    pair_count = N_GA // 2
    shifts = jax.random.randint(key_pairs, (pair_count,), -dead_mean, dead_mean + 1).astype(jnp.int32)
    shifts = shifts.at[0].set(dead_mean)
    dead_slots = jnp.concatenate([dead_mean + shifts, dead_mean - shifts])
    dead_slots = jax.random.permutation(key_order, dead_slots)
    counts = (SLOT_DEV - dead_slots).astype(jnp.int32)
    offsets = jnp.cumsum(counts) - counts
    slot_ids = jnp.arange(SLOT_DEV, dtype=jnp.int32)
    slot_pos = jnp.clip(offsets[:, None] + slot_ids[None, :], 0, NPW - 1)
    live_mask = slot_ids[None, :] < counts[:, None]
    filler = jax.random.randint(key_dead, (N_GA, SLOT_DEV), 0, cell_count).astype(jnp.int32)
    index_map = jnp.where(live_mask, ball_cells[slot_pos], filler).reshape(-1).astype(jnp.int32)
    return (index_map, counts)


def draw_index_map(key, part):
    return layout_draw(key)[0]


def draw_counts(key, part):
    return layout_draw(key)[1]


def spiked(entries, rng, source, target, shards_of, factor):
    owner, partner = [(jnp.arange(entries.shape[dim]) // (entries.shape[dim] // shards_of)).reshape([-1 if axis == dim else 1 for axis in range(entries.ndim)]) for dim in (source, target)]
    chosen = jax.random.permutation(rng, shards_of)[partner]
    strong = (owner == chosen) | (owner == (partner + shards_of // 2) % shards_of)
    return jnp.where(strong, factor * entries, entries)


def level_of(own_key, extent, cuts, least, largest):
    level = 1.0
    for axis_at, shards_of in cuts:
        draws = jax.random.uniform(jax.random.fold_in(jax.random.fold_in(own_key, 6), axis_at), (shards_of,), jnp.float32, least / len(cuts), largest / len(cuts))
        level = level * jnp.repeat(jnp.exp(draws), extent[axis_at] // shards_of).reshape((-1,) + (1,) * (len(extent) - 1 - axis_at))
    return level


def normal_values(rng, extent, deviation, limit, pieces=(), held_as=jnp.bfloat16):
    values = deviation * jax.random.normal(rng, extent, jnp.float32)
    if pieces:
        values = values * level_of(rng, extent, pieces, -0.22, 0.18)
    return jnp.clip(values, -limit, limit).astype(held_as)


def noise_with(key, dims, width, limit, pieces, heavy, kind=jnp.bfloat16):
    result = width * jax.random.normal(key, dims, jnp.float32)
    if pieces:
        result = result * level_of(key, dims, pieces, -0.22, 0.18)
    return jnp.clip(spiked(result, jax.random.fold_in(key, 3), *heavy), -limit, limit).astype(kind)


def setup_inputs(seed: int = 0) -> dict:
    streams_of = jax.random.split(jax.random.key(seed), 6)
    coefficients = normal_values(streams_of[0], (BANDS, 2, SLOT_DEV * N_GA), 1.0, 6.0, ((0, 2), (2, 16)), jnp.float32)
    rotation = noise_with(streams_of[1], (2, BANDS, PANEL), (2 * BANDS) ** -0.5, 0.125, ((1, 2), (2, 16)), (1, 2, 16, 2.0), jnp.float32)
    potential = jnp.clip(-2.0 + 2.5 * jax.random.uniform(streams_of[2], (BOX, BOX * BOX), jnp.float32) ** level_of(streams_of[2], (BOX, BOX * BOX), ((1, 16),), -0.2, 0.2), -2.0, 0.5)
    index_map = draw_index_map(jax.random.fold_in(streams_of[5], 71), 0)
    counts = draw_counts(jax.random.fold_in(streams_of[5], 71), 0)
    return {"coefficients": coefficients, "rotation": rotation, "potential": potential, "index_map": index_map, "counts": counts}


def mixing(columns):
    real_cols = columns[0].T
    imag_cols = columns[1].T
    upper_rows = jnp.stack([real_cols, -imag_cols], axis=-1)
    lower_rows = jnp.stack([imag_cols, real_cols], axis=-1)
    stacked = jnp.stack([upper_rows, lower_rows], axis=1)
    return stacked.reshape(2 * real_cols.shape[0], 2 * real_cols.shape[1])


def kinetic_grid(box_edge):
    ticks_index = jnp.arange(box_edge, dtype=jnp.int32)
    signed = jnp.where(ticks_index >= box_edge // 2, ticks_index - box_edge, ticks_index).astype(jnp.float32)
    squared = signed[:, None, None] ** 2 + signed[None, :, None] ** 2 + signed[None, None, :] ** 2
    return (8.0 / (box_edge * box_edge)) * squared


def reference(coefficients, rotation, potential, index_map, counts):
    band_count = coefficients.shape[0]
    slot_total = coefficients.shape[2]
    mixer_rows = mixing(rotation)
    rotated = jnp.dot(mixer_rows, coefficients.reshape(2 * band_count, slot_total),
                      precision=lax.Precision.HIGHEST).reshape(PANEL, 2, slot_total)
    slot_ids = jnp.arange(SLOT_DEV, dtype=jnp.int32)
    live_mask = (slot_ids[None, :] < counts[:, None]).reshape(-1).astype(jnp.float32)
    kinetic = kinetic_grid(BOX)
    pot_grid = potential.reshape(BOX, BOX, BOX)
    window = BOX // 2
    window_ids = ((jnp.arange(window, dtype=jnp.int32) - window // 2) % BOX).astype(jnp.int32)

    def one_band(values):
        masked = values * live_mask[None, :]
        box_cells = jnp.zeros((2, BOX * BOX * BOX), jnp.float32).at[:, index_map].add(masked)
        grid_field = (box_cells[0] + 1j * box_cells[1]).reshape(BOX, BOX, BOX)
        real_space = jnp.fft.ifftn(grid_field)
        applied = jnp.fft.fftn(pot_grid * real_space) + kinetic * grid_field
        applied = jnp.take(applied, window_ids, axis=0)
        applied = jnp.take(applied, window_ids, axis=1)
        applied = jnp.take(applied, window_ids, axis=2)
        return jnp.stack([applied.real, applied.imag]).reshape(2, window, window * window)

    return lax.map(one_band, rotated)
```

```python
import functools
import math

import jax
import jax.numpy as jnp
import numpy as np
from jax import lax
from jax.experimental import pallas as pl
from jax.experimental.pallas import tpu as pltpu
from jax.sharding import PartitionSpec as P

F32 = jnp.float32
BF16 = jnp.bfloat16
I32 = jnp.int32
MESH = pl.DeviceIdType.MESH


def split_parts(values):
    high = values.astype(BF16)
    return high, (values - high.astype(F32)).astype(BF16)


def two_parts(table):
    high = table.astype(BF16)
    low = (table - high.astype(np.float32)).astype(BF16)
    return np.stack([high, low])


class Sizes:
    def __init__(self, box, window):
        self.box, self.window, self.half = box, window, window // 2
        self.low = 4
        self.high = window // self.low
        self.span = box // self.low
        self.rows = self.low * window
        self.cols = self.high * window
        self.wide = self.span * box
        self.deep = self.low * box
        self.fold = 2
        self.lanes = self.cols // self.fold
        assert box % self.low == 0 and box == 2 * window and box & (box - 1) == 0


def tables(sz):
    n_signed = np.arange(sz.window) - sz.half
    k_all = np.arange(sz.box)
    y_start = sz.low * np.arange(sz.high) - sz.half
    k_low = np.arange(sz.span)
    digit = np.arange(sz.low)

    def pair(phase):
        angle = (phase % sz.box) * (2.0 * math.pi / sz.box)
        return np.stack([np.cos(angle), np.sin(angle)])

    y_phase = y_start[:, None] * k_low[None, :]
    z_phase = n_signed[:, None] * k_all[None, :]
    base = np.concatenate(
        [pair(np.tile(z_phase, (1, sz.span))), pair(np.repeat(y_phase, sz.box, axis=1))], axis=1
    )
    flip = np.concatenate(
        [pair(np.tile(z_phase.T, (1, sz.high))), pair(np.repeat(y_phase.T, sz.window, axis=1))], axis=1
    )
    twist = pair(np.repeat(digit[:, None] * k_low[None, :], sz.box, axis=1))
    l_phase = sz.span * digit[:, None] * digit[None, :]
    x_phase = k_all[:, None] * n_signed[None, :]
    left = (l_phase[:, None, :, None] + x_phase[None, :, None, :]).reshape(sz.deep, sz.rows)
    cos, sin = pair(left)
    fore = two_parts((np.block([[cos, -sin], [sin, cos]]) / sz.box**3).astype(np.float32))
    back = two_parts(np.block([[cos.T, sin.T], [-sin.T, cos.T]]).astype(np.float32))
    return base.astype(np.float32), flip.astype(np.float32), twist.astype(np.float32), fore, back


def dot(a, b, dims=((1,), (0,))):
    return lax.dot_general(a, b, (dims, ((), ())), preferred_element_type=F32)


def whole_kernel(
    bands, groups, sz, early, coef_hbm, rot_hbm, pot_hbm, idx_hbm, cnt_hbm, base_hbm, flip_hbm, twist_hbm,
    fore_hbm, back_hbm, out_ref, coef, rot_ref, idx, cnt, base, flip, twist, fore, back, right, right_t,
    rows_hot, cols_hot, parts, rots, prod, land, pot, grid, space, kin, load_sem, self_sem, rot_send,
    rot_recv, pot_send, pot_recv, pass_send, pass_recv, val_send, val_recv
):
    band = lax.axis_index("band")
    me = lax.axis_index("ga")
    flat = band * groups + me
    depth, slots = coef.shape[1], coef.shape[2]
    cols = rot_ref.shape[1]
    panel = groups * cols
    own = land.shape[1]
    share_rows = pot_hbm.shape[0] // bands

    def share(holder):
        return pl.ds(pl.multiple_of(holder * share_rows, share_rows), share_rows)

    def load(src, dst, at):
        return pltpu.make_async_copy(src, dst, load_sem.at[at])

    rot_load = load(rot_hbm, rot_ref, 0)
    rot_load.start()
    small = [
        load(src, dst, at + 1)
        for at, (src, dst) in enumerate(
            (
                (base_hbm, base), (flip_hbm, flip), (idx_hbm, idx), (cnt_hbm, cnt), (twist_hbm, twist),
                (fore_hbm, fore), (back_hbm, back),
            )
        )
    ]
    coef_load = [load(coef_hbm.at[:, c, :], coef.at[c], 8 + c) for c in range(2)]
    for item in small[:4] + coef_load + small[4:]:
        item.start()

    barrier = pltpu.get_barrier_semaphore()
    peers = [(db, dg) for db in range(bands) for dg in range(groups) if db or dg]

    def ahead(db, dg):
        return {"band": lax.rem(band + db, bands), "ga": lax.rem(me + dg, groups)}

    def every(act):
        if len(peers) < 64:
            for db, dg in peers:
                act(db, dg)
        else:

            def body(step, carry):
                act(step // groups, lax.rem(step, groups))
                return carry

            lax.fori_loop(1, bands * groups, body, 0)

    def greet(db, dg):
        pl.semaphore_signal(barrier, inc=1, device_id=ahead(db, dg), device_id_type=MESH)

    every(greet)
    rot_load.wait()
    rot_self = pltpu.make_async_copy(rot_hbm, rots.at[me], self_sem.at[0])
    rot_self.start()
    pot_self = pltpu.make_async_copy(pot_hbm.at[share(band)], pot.at[0, share(band)], self_sem.at[1])
    pot_self.start()
    pl.semaphore_wait(barrier, bands * groups - 1)

    def rot_copy(step):
        return pltpu.make_async_remote_copy(
            src_ref=rot_ref, dst_ref=rots.at[me], send_sem=rot_send.at[step], recv_sem=rot_recv.at[step],
            device_id={"band": band, "ga": lax.rem(me + step, groups)}, device_id_type=MESH,
        )

    def pot_copy(step):
        return pltpu.make_async_remote_copy(
            src_ref=pot_hbm.at[share(band)], dst_ref=pot.at[step, share(band)],
            send_sem=pot_send.at[step], recv_sem=pot_recv.at[step],
            device_id={"band": band, "ga": lax.rem(me + step, groups)}, device_id_type=MESH,
        )

    def pass_copy(piece, db, holder):
        held = pot.at[pl.ds(piece[0], piece[1] - piece[0]), share(holder)]
        return pltpu.make_async_remote_copy(
            src_ref=held, dst_ref=held, send_sem=pass_send.at[db, piece[2]], recv_sem=pass_recv.at[db, piece[2]],
            device_id={"band": lax.rem(band + db, bands), "ga": me}, device_id_type=MESH,
        )

    def val_copy(db, dg):
        to = ahead(db, dg)
        return pltpu.make_async_remote_copy(
            src_ref=prod.at[pl.ds((to["band"] * groups + to["ga"]) * own, own)], dst_ref=land.at[db * groups + dg],
            send_sem=val_send.at[db * groups + dg], recv_sem=val_recv.at[db * groups + dg],
            device_id=to, device_id_type=MESH,
        )

    pieces = [(0, early, 0), (early, groups, 1)]
    for step in range(1, groups):
        rot_copy(step).start()
    for step in range(1, early):
        pot_copy(step).start()

    small[0].wait()

    def fill_right(step, carry):
        at = pl.multiple_of(step * sz.window, sz.window)
        y_cos = base[0, pl.ds(sz.window + step, 1), :]
        y_sin = base[1, pl.ds(sz.window + step, 1), :]
        z_cos, z_sin = base[0, : sz.window, :], base[1, : sz.window, :]
        cos = split_parts(z_cos * y_cos - z_sin * y_sin)
        sin = split_parts(z_sin * y_cos + z_cos * y_sin)
        for part in range(2):
            right[part, pl.ds(at, sz.window), : sz.wide] = cos[part]
            right[part, pl.ds(at, sz.window), sz.wide :] = sin[part]
            right[part, pl.ds(sz.cols + at, sz.window), : sz.wide] = -sin[part]
            right[part, pl.ds(sz.cols + at, sz.window), sz.wide :] = cos[part]
        return carry

    lax.fori_loop(0, sz.high, fill_right, 0)
    small[1].wait()

    def fill_right_t(step, carry):
        at = pl.multiple_of(step * sz.box, sz.box)
        y_cos = flip[0, pl.ds(sz.box + step, 1), :]
        y_sin = flip[1, pl.ds(sz.box + step, 1), :]
        z_cos, z_sin = flip[0, : sz.box, :], flip[1, : sz.box, :]
        cos = split_parts(z_cos * y_cos - z_sin * y_sin)
        sin = split_parts(z_sin * y_cos + z_cos * y_sin)
        for part in range(2):
            right_t[part, pl.ds(at, sz.box), : sz.cols] = cos[part]
            right_t[part, pl.ds(at, sz.box), sz.cols :] = -sin[part]
            right_t[part, pl.ds(sz.wide + at, sz.box), : sz.cols] = sin[part]
            right_t[part, pl.ds(sz.wide + at, sz.box), sz.cols :] = cos[part]
        return carry

    lax.fori_loop(0, sz.span, fill_right_t, 0)
    small[2].wait()
    small[3].wait()
    bits = sz.box.bit_length() - 1

    def fill_hot(step, carry):
        at = pl.ds(pl.multiple_of(step * slots, slots), slots)
        cell = idx[:, at]
        n_x = (jnp.right_shift(cell, 2 * bits) + sz.half) & (sz.box - 1)
        n_y = (jnp.right_shift(cell, bits) + sz.half) & (sz.box - 1)
        n_z = (cell + sz.half) & (sz.box - 1)
        live = lax.broadcasted_iota(I32, (1, slots), 1) < cnt[step]
        live = live & (n_x < sz.window) & (n_y < sz.window) & (n_z < sz.window)
        y_high, y_low = n_y // sz.low, n_y % sz.low
        block, fine = y_high // (sz.high // sz.fold), y_high % (sz.high // sz.fold)
        row = jnp.where(live, block * sz.rows + y_low * sz.window + n_x, -1)
        col = fine * sz.window + n_z
        row_at = lax.broadcasted_iota(I32, (sz.fold * sz.rows, slots), 0)
        col_at = lax.broadcasted_iota(I32, (sz.lanes, slots), 0)
        rows_hot[:, at] = jnp.where(row_at == row, 1.0, 0.0).astype(BF16)
        cols_hot[:, at] = jnp.where(col_at == col, 1.0, 0.0).astype(BF16)
        return carry

    lax.fori_loop(0, groups, fill_hot, 0)
    row_at = lax.broadcasted_iota(I32, (sz.rows, sz.cols), 0)
    col_at = lax.broadcasted_iota(I32, (sz.rows, sz.cols), 1)
    n_x = (row_at % sz.window - sz.half).astype(F32)
    n_y = (col_at // sz.window * sz.low + row_at // sz.window - sz.half).astype(F32)
    n_z = (col_at % sz.window - sz.half).astype(F32)
    kin[...] = (8.0 / (sz.box * sz.box)) * (n_x * n_x + n_y * n_y + n_z * n_z)

    slab = 128
    for c in range(2):
        coef_load[c].wait()

        def fill_parts(step, carry, c=c):
            at = pl.multiple_of(step * slab, slab)
            high, low = split_parts(coef[c, pl.ds(at, slab), :])
            parts[0, pl.ds(c * depth + at, slab), :] = high
            parts[1, pl.ds(c * depth + at, slab), :] = low
            return carry

        lax.fori_loop(0, depth // slab, fill_parts, 0)
    for item in small[4:]:
        item.wait()

    rot_self.wait()
    for step in range(1, groups):
        rot_copy(step).wait_recv()
    real = rots[:, 0].reshape(panel, depth)
    imag = rots[:, 1].reshape(panel, depth)
    mixer = jnp.concatenate(
        [jnp.concatenate([real, -imag], axis=1), jnp.concatenate([imag, real], axis=1)], axis=0
    )
    high, low = split_parts(mixer)
    first = dot(jnp.concatenate([high, low], axis=0), parts[0])
    mixed = first[: 2 * panel] + first[2 * panel :] + dot(high, parts[1])
    prod[:, 0, :] = mixed[:panel]
    prod[:, 1, :] = mixed[panel:]

    every(lambda db, dg: val_copy(db, dg).start())
    val_self = prod.at[pl.ds(flat * own, own)]
    for step in range(early, groups):
        pot_copy(step).start()

    def relay(piece):
        for step in range(max(piece[0], 1), piece[1]):
            pot_copy(step).wait_recv()
        for db in range(1, bands):
            pass_copy(piece, db, band).start()

    pot_self.wait()
    relay(pieces[0])

    batch = 4 if groups % 4 == 0 else 1
    for i in range(own):
        for start in range(0, groups, batch):
            total = None
            for dg in range(start, start + batch):
                values = val_self[i] if dg == 0 else None
                for db in range(bands):
                    if i == 0 and (db or dg):
                        val_copy(db, dg).wait_recv()
                    if db or dg:
                        piece = land[db * groups + dg, i]
                        values = piece if values is None else values + piece
                source = lax.rem(me + groups - dg, groups)
                at = pl.ds(pl.multiple_of(source * slots, slots), slots)
                hits = cols_hot[:, at]
                placed = jnp.concatenate(
                    [hits * part[c : c + 1, :] for part in split_parts(values) for c in range(2)], axis=0
                )
                term = dot(rows_hot[:, at], placed, ((1,), (1,)))
                total = term if total is None else total + term
            if start:
                grid[...] += total
            else:
                grid[...] = total
        if i == 0:
            relay(pieces[1])

        def pot_ready():
            for piece in pieces:
                for db in range(1, bands):
                    pass_copy(piece, db, lax.rem(band + bands - db, bands)).wait_recv()

        apply_kernel(
            groups, sz, i, me, pot_ready if i == 0 else None, grid, pot, right, right_t, fore, back, twist, kin, space, out_ref
        )
    every(lambda db, dg: val_copy(db, dg).wait_send())
    for step in range(1, groups):
        rot_copy(step).wait_send()
        pot_copy(step).wait_send()
    for piece in pieces:
        for db in range(1, bands):
            pass_copy(piece, db, band).wait_send()


def apply_kernel(
    groups, sz, index, me, pot_ready, grid, pot, right, right_t, fore, back, twist, kin, space, out_ref
):
    whole = 2 * sz.lanes
    summed = grid[:, :whole] + grid[:, whole:]
    field = jnp.concatenate(
        [
            summed[f * sz.rows : (f + 1) * sz.rows, c * sz.lanes : (c + 1) * sz.lanes]
            for c in range(2)
            for f in range(sz.fold)
        ],
        axis=1,
    )
    field_high, field_low = split_parts(field)
    step = 256
    for at in range(0, sz.wide, step):
        halves = []
        for c in range(2):
            here = slice(c * sz.wide + at, c * sz.wide + at + step)
            halves.append(
                dot(field_high, right[0, :, here])
                + (dot(field_low, right[0, :, here]) + dot(field_high, right[1, :, here]))
            )
        real = halves[0].reshape(sz.low, sz.window, step)
        imag = halves[1].reshape(sz.low, sz.window, step)
        cos = twist[0, :, at : at + step][:, None, :]
        sin = twist[1, :, at : at + step][:, None, :]
        turned = jnp.concatenate(
            [
                (real * cos - imag * sin).reshape(sz.rows, step),
                (real * sin + imag * cos).reshape(sz.rows, step),
            ],
            axis=0,
        )
        high, low = split_parts(turned)
        space[:, at : at + step] = dot(fore[0], high) + (dot(fore[0], low) + dot(fore[1], high))
    if pot_ready is not None:
        pot_ready()
    each = pot.shape[2]
    per = groups // sz.low
    applied = None
    for at in range(0, sz.wide, step):
        blocks = []
        for k_high in range(sz.low):
            lane = []
            for q in range(at // each, (at + step + each - 1) // each):
                lane.append(pot[lax.rem(me + groups - (k_high * per + q), groups)])
            blocks.append(lane[0] if len(lane) == 1 else jnp.concatenate(lane, axis=1))
        local = jnp.concatenate(blocks, axis=0)
        high, low = split_parts(space[:, at : at + step] * jnp.concatenate([local, local], axis=0))
        spread = dot(back[0], high) + (dot(back[0], low) + dot(back[1], high))
        real = spread[: sz.rows].reshape(sz.low, sz.window, step)
        imag = spread[sz.rows :].reshape(sz.low, sz.window, step)
        cos = twist[0, :, at : at + step][:, None, :]
        sin = twist[1, :, at : at + step][:, None, :]
        turned = [
            (real * cos + imag * sin).reshape(sz.rows, step),
            (imag * cos - real * sin).reshape(sz.rows, step),
        ]
        for c in range(2):
            here = slice(c * sz.wide + at, c * sz.wide + at + step)
            high, low = split_parts(turned[c])
            term = dot(high, right_t[0, here, :]) + (
                dot(low, right_t[0, here, :]) + dot(high, right_t[1, here, :])
            )
            applied = term if applied is None else applied + term
    applied = applied + jnp.concatenate([kin[...], kin[...]], axis=1) * field
    for c in range(2):
        pieces = [
            applied[lo * sz.window : (lo + 1) * sz.window, c * sz.cols + hi * sz.window : c * sz.cols + (hi + 1) * sz.window]
            for hi in range(sz.high)
            for lo in range(sz.low)
        ]
        out_ref[index, c] = jnp.concatenate(pieces, axis=1)


def run(coefficients, rotation, potential, index_map, counts, box, early):
    bands, groups = lax.axis_size("band"), lax.axis_size("ga")
    sz = Sizes(box, box // 2)
    depth, _, slots = coefficients.shape
    cols = rotation.shape[2]
    panel = cols * groups
    own = panel // (bands * groups)
    consts = [jnp.asarray(t) for t in tables(sz)]
    hbm = pl.BlockSpec(memory_space=pl.ANY)
    dma = pltpu.SemaphoreType.DMA
    return pl.pallas_call(
        functools.partial(whole_kernel, bands, groups, sz, early),
        out_shape=jax.ShapeDtypeStruct((own, 2, sz.window, sz.window * sz.window), F32),
        in_specs=[hbm] * 10,
        out_specs=pl.BlockSpec(memory_space=pltpu.VMEM),
        scratch_shapes=[
            pltpu.VMEM((2, depth, slots), F32),
            pltpu.VMEM((2, cols, depth), F32),
            pltpu.VMEM((1, index_map.shape[0]), I32),
            pltpu.SMEM(counts.shape, I32),
            *[pltpu.VMEM(table.shape, table.dtype) for table in consts],
            pltpu.VMEM((2, 2 * sz.cols, 2 * sz.wide), BF16),
            pltpu.VMEM((2, 2 * sz.wide, 2 * sz.cols), BF16),
            pltpu.VMEM((sz.fold * sz.rows, index_map.shape[0]), BF16),
            pltpu.VMEM((sz.lanes, index_map.shape[0]), BF16),
            pltpu.VMEM((2, 2 * depth, slots), BF16),
            pltpu.VMEM((groups, 2, cols, depth), F32),
            pltpu.VMEM((panel, 2, slots), F32),
            pltpu.VMEM((bands * groups, own, 2, slots), F32),
            pltpu.VMEM((groups,) + potential.shape, F32),
            pltpu.VMEM((sz.fold * sz.rows, 4 * sz.lanes), F32),
            pltpu.VMEM((2 * sz.deep, sz.wide), F32),
            pltpu.VMEM((sz.rows, sz.cols), F32),
            dma((10,)),
            dma((2,)),
            dma((groups,)),
            dma((groups,)),
            dma((groups,)),
            dma((groups,)),
            dma((bands, 2)),
            dma((bands, 2)),
            dma((bands * groups,)),
            dma((bands * groups,)),
        ],
        compiler_params=pltpu.CompilerParams(
            collective_id=0, has_side_effects=True, vmem_limit_bytes=60 * 1024 * 1024
        ),
    )(coefficients, rotation.transpose(0, 2, 1), potential, index_map[None], counts, *consts)


def per_device(coefficients, rotation, potential, index_map, counts):
    groups = lax.axis_size("ga")
    return run(coefficients, rotation, potential, index_map, counts, potential.shape[0], groups // 2)


def solution(mesh):
    placed = (P("band", None, "ga"), P(None, "band", "ga"), P(None, "ga"), P(), P())
    return jax.shard_map(
        per_device,
        mesh=mesh,
        in_specs=placed,
        out_specs=P(("band", "ga"), None, None, None),
        check_vma=False,
    )
```

```python
import functools
import math

import jax
import jax.numpy as jnp
import numpy as np
from jax import lax
from jax.experimental import pallas as pl
from jax.experimental.pallas import tpu as pltpu
from jax.sharding import PartitionSpec as P

F32 = jnp.float32
BF16 = jnp.bfloat16
I32 = jnp.int32
MESH = pl.DeviceIdType.MESH


def split_parts(values):
    high = values.astype(BF16)
    return high, (values - high.astype(F32)).astype(BF16)


def two_parts(table):
    high = table.astype(BF16)
    low = (table - high.astype(np.float32)).astype(BF16)
    return np.stack([high, low])


class Sizes:
    def __init__(self, box, window):
        self.box, self.window, self.half = box, window, window // 2
        self.low = 4
        self.high = window // self.low
        self.span = box // self.low
        self.rows = self.low * window
        self.cols = self.high * window
        self.wide = self.span * box
        self.deep = self.low * box
        self.fold = 2
        self.lanes = self.cols // self.fold
        assert box % self.low == 0 and box == 2 * window and box & (box - 1) == 0


def tables(sz):
    n_signed = np.arange(sz.window) - sz.half
    k_all = np.arange(sz.box)
    y_start = sz.low * np.arange(sz.high) - sz.half
    k_low = np.arange(sz.span)
    digit = np.arange(sz.low)

    def pair(phase):
        angle = (phase % sz.box) * (2.0 * math.pi / sz.box)
        return np.stack([np.cos(angle), np.sin(angle)])

    y_phase = y_start[:, None] * k_low[None, :]
    z_phase = n_signed[:, None] * k_all[None, :]
    base = np.concatenate(
        [pair(np.tile(z_phase, (1, sz.span))), pair(np.repeat(y_phase, sz.box, axis=1))], axis=1
    )
    flip = np.concatenate(
        [pair(np.tile(z_phase.T, (1, sz.high))), pair(np.repeat(y_phase.T, sz.window, axis=1))], axis=1
    )
    twist = pair(np.repeat(digit[:, None] * k_low[None, :], sz.box, axis=1))
    l_phase = sz.span * digit[:, None] * digit[None, :]
    x_phase = k_all[:, None] * n_signed[None, :]
    left = (l_phase[:, None, :, None] + x_phase[None, :, None, :]).reshape(sz.deep, sz.rows)
    cos, sin = pair(left)
    fore = two_parts((np.block([[cos, -sin], [sin, cos]]) / sz.box**3).astype(np.float32))
    back = two_parts(np.block([[cos.T, sin.T], [-sin.T, cos.T]]).astype(np.float32))
    return base.astype(np.float32), flip.astype(np.float32), twist.astype(np.float32), fore, back


def dot(a, b, dims=((1,), (0,))):
    return lax.dot_general(a, b, (dims, ((), ())), preferred_element_type=F32)


def whole_kernel(
    bands, groups, sz, coef_hbm, rot_hbm, pot_hbm, idx_hbm, cnt_hbm, base_hbm, flip_hbm, twist_hbm,
    fore_hbm, back_hbm, out_ref, coef, rot_ref, idx, cnt, base, flip, twist, fore, back, right, right_t,
    rows_hot, cols_hot, parts, rots, prod, land, pot, grid, space, kin, load_sem, self_sem, rot_send,
    rot_recv, pot_send, pot_recv, pass_send, pass_recv, val_send, val_recv
):
    band = lax.axis_index("band")
    me = lax.axis_index("ga")
    flat = band * groups + me
    depth, slots = coef.shape[1], coef.shape[2]
    cols = rot_ref.shape[1]
    panel = groups * cols
    own = land.shape[1]
    share_rows = pot_hbm.shape[0] // bands

    def share(holder):
        return pl.ds(pl.multiple_of(holder * share_rows, share_rows), share_rows)

    def load(src, dst, at):
        return pltpu.make_async_copy(src, dst, load_sem.at[at])

    rot_load = load(rot_hbm, rot_ref, 0)
    rot_load.start()
    small = [
        load(src, dst, at + 1)
        for at, (src, dst) in enumerate(
            (
                (base_hbm, base), (flip_hbm, flip), (idx_hbm, idx), (cnt_hbm, cnt), (twist_hbm, twist),
                (fore_hbm, fore), (back_hbm, back),
            )
        )
    ]
    coef_load = [load(coef_hbm.at[:, c, :], coef.at[c], 8 + c) for c in range(2)]
    for item in small[:4] + coef_load + small[4:]:
        item.start()

    near = 4 if groups % 4 == 0 else 1
    lines = groups // near
    assert groups & (groups - 1) == 0

    def flip_bits(value, mask, count):
        total, bit = 0, 1
        while bit < count:
            ours, theirs = lax.rem(value // bit, 2), lax.rem(mask // bit, 2) if not isinstance(mask, int) else mask // bit % 2
            total = total + bit * (ours + theirs - 2 * ours * theirs)
            bit *= 2
        return total

    def peer(step):
        return flip_bits(me, step, groups)

    barrier = pltpu.get_barrier_semaphore()
    hops = [(0, near * z) for z in range(1, lines)] + [(0, p) for p in range(1, near)]
    hops += [(db, 0) for db in range(1, bands)]

    def ahead(db, step):
        return {"band": lax.rem(band + db, bands), "ga": peer(step)}

    for db, step in hops:
        pl.semaphore_signal(barrier, inc=1, device_id=ahead(db, step), device_id_type=MESH)
    rot_load.wait()
    rot_self = pltpu.make_async_copy(rot_hbm, rots.at[me], self_sem.at[0])
    rot_self.start()
    pot_self = pltpu.make_async_copy(pot_hbm.at[share(band)], pot.at[0, share(band)], self_sem.at[1])
    pot_self.start()
    pl.semaphore_wait(barrier, len(hops))

    def rot_copy(z, p):
        slot = peer(near * z) if p else me
        return pltpu.make_async_remote_copy(
            src_ref=rots.at[slot] if z and p else rot_ref, dst_ref=rots.at[slot],
            send_sem=rot_send.at[near * z + p], recv_sem=rot_recv.at[near * z + p],
            device_id=ahead(0, p if p else near * z), device_id_type=MESH,
        )

    def pot_line(z):
        return pltpu.make_async_remote_copy(
            src_ref=pot_hbm.at[share(band)], dst_ref=pot.at[z, share(band)],
            send_sem=pot_send.at[z], recv_sem=pot_recv.at[z],
            device_id=ahead(0, near * z), device_id_type=MESH,
        )

    def pot_plane(p):
        return pltpu.make_async_remote_copy(
            src_ref=pot.at[pl.ds(0, lines), share(band)], dst_ref=pot.at[pl.ds(p * lines, lines), share(band)],
            send_sem=pot_send.at[lines + p], recv_sem=pot_recv.at[lines + p],
            device_id=ahead(0, p), device_id_type=MESH,
        )

    def pass_copy(p, db, holder):
        held = pot.at[pl.ds(p * lines, lines), share(holder)]
        return pltpu.make_async_remote_copy(
            src_ref=held, dst_ref=held, send_sem=pass_send.at[db, p], recv_sem=pass_recv.at[db, p],
            device_id=ahead(db, 0), device_id_type=MESH,
        )

    def val_copy(db, step):
        to = ahead(db, step)
        at = db * groups + step
        return pltpu.make_async_remote_copy(
            src_ref=prod.at[pl.ds((to["band"] * groups + to["ga"]) * own, own)], dst_ref=land.at[at],
            send_sem=val_send.at[at], recv_sem=val_recv.at[at], device_id=to, device_id_type=MESH,
        )

    def pot_slot(ga):
        step = peer(ga)
        return lax.rem(step, near) * lines + step // near

    def every(act):
        if bands * groups <= 64:
            for step in reversed(range(groups)):
                for db in range(bands):
                    if db or step:
                        act(db, step)
        else:

            def body(at, carry):
                act(at // groups, lax.rem(at, groups))
                return carry

            lax.fori_loop(1, bands * groups, body, 0)

    for z in range(1, lines):
        rot_copy(z, 0).start()
    for p in range(1, near):
        rot_copy(0, p).start()

    small[0].wait()

    def fill_right(step, carry):
        at = pl.multiple_of(step * sz.window, sz.window)
        y_cos = base[0, pl.ds(sz.window + step, 1), :]
        y_sin = base[1, pl.ds(sz.window + step, 1), :]
        z_cos, z_sin = base[0, : sz.window, :], base[1, : sz.window, :]
        cos = split_parts(z_cos * y_cos - z_sin * y_sin)
        sin = split_parts(z_sin * y_cos + z_cos * y_sin)
        for part in range(2):
            right[part, pl.ds(at, sz.window), : sz.wide] = cos[part]
            right[part, pl.ds(at, sz.window), sz.wide :] = sin[part]
            right[part, pl.ds(sz.cols + at, sz.window), : sz.wide] = -sin[part]
            right[part, pl.ds(sz.cols + at, sz.window), sz.wide :] = cos[part]
        return carry

    lax.fori_loop(0, sz.high, fill_right, 0)
    for z in range(1, lines):
        pot_line(z).start()
    small[1].wait()

    def fill_right_t(step, carry):
        at = pl.multiple_of(step * sz.box, sz.box)
        y_cos = flip[0, pl.ds(sz.box + step, 1), :]
        y_sin = flip[1, pl.ds(sz.box + step, 1), :]
        z_cos, z_sin = flip[0, : sz.box, :], flip[1, : sz.box, :]
        cos = split_parts(z_cos * y_cos - z_sin * y_sin)
        sin = split_parts(z_sin * y_cos + z_cos * y_sin)
        for part in range(2):
            right_t[part, pl.ds(at, sz.box), : sz.cols] = cos[part]
            right_t[part, pl.ds(at, sz.box), sz.cols :] = -sin[part]
            right_t[part, pl.ds(sz.wide + at, sz.box), : sz.cols] = sin[part]
            right_t[part, pl.ds(sz.wide + at, sz.box), sz.cols :] = cos[part]
        return carry

    lax.fori_loop(0, sz.span, fill_right_t, 0)
    for z in range(1, lines):
        rot_copy(z, 0).wait_recv()
        for p in range(1, near):
            rot_copy(z, p).start()
    small[2].wait()
    small[3].wait()
    bits = sz.box.bit_length() - 1

    def fill_hot(step, carry):
        at = pl.ds(pl.multiple_of(step * slots, slots), slots)
        cell = idx[:, at]
        n_x = (jnp.right_shift(cell, 2 * bits) + sz.half) & (sz.box - 1)
        n_y = (jnp.right_shift(cell, bits) + sz.half) & (sz.box - 1)
        n_z = (cell + sz.half) & (sz.box - 1)
        live = lax.broadcasted_iota(I32, (1, slots), 1) < cnt[step]
        live = live & (n_x < sz.window) & (n_y < sz.window) & (n_z < sz.window)
        y_high, y_low = n_y // sz.low, n_y % sz.low
        block, fine = y_high // (sz.high // sz.fold), y_high % (sz.high // sz.fold)
        row = jnp.where(live, block * sz.rows + y_low * sz.window + n_x, -1)
        col = fine * sz.window + n_z
        row_at = lax.broadcasted_iota(I32, (sz.fold * sz.rows, slots), 0)
        col_at = lax.broadcasted_iota(I32, (sz.lanes, slots), 0)
        rows_hot[:, at] = jnp.where(row_at == row, 1.0, 0.0).astype(BF16)
        cols_hot[:, at] = jnp.where(col_at == col, 1.0, 0.0).astype(BF16)
        return carry

    lax.fori_loop(0, groups, fill_hot, 0)
    row_at = lax.broadcasted_iota(I32, (sz.rows, sz.cols), 0)
    col_at = lax.broadcasted_iota(I32, (sz.rows, sz.cols), 1)
    n_x = (row_at % sz.window - sz.half).astype(F32)
    n_y = (col_at // sz.window * sz.low + row_at // sz.window - sz.half).astype(F32)
    n_z = (col_at % sz.window - sz.half).astype(F32)
    kin[...] = (8.0 / (sz.box * sz.box)) * (n_x * n_x + n_y * n_y + n_z * n_z)

    slab = 128
    for c in range(2):
        coef_load[c].wait()

        def fill_parts(step, carry, c=c):
            at = pl.multiple_of(step * slab, slab)
            high, low = split_parts(coef[c, pl.ds(at, slab), :])
            parts[0, pl.ds(c * depth + at, slab), :] = high
            parts[1, pl.ds(c * depth + at, slab), :] = low
            return carry

        lax.fori_loop(0, depth // slab, fill_parts, 0)
    for item in small[4:]:
        item.wait()

    rot_self.wait()
    for z in range(lines):
        for p in range(1, near):
            rot_copy(z, p).wait_recv()
    real = rots[:, 0].reshape(panel, depth)
    imag = rots[:, 1].reshape(panel, depth)
    mixer = jnp.concatenate(
        [jnp.concatenate([real, -imag], axis=1), jnp.concatenate([imag, real], axis=1)], axis=0
    )
    high, low = split_parts(mixer)
    first = dot(jnp.concatenate([high, low], axis=0), parts[0])
    mixed = first[: 2 * panel] + first[2 * panel :] + dot(high, parts[1])
    prod[:, 0, :] = mixed[:panel]
    prod[:, 1, :] = mixed[panel:]

    every(lambda db, step: val_copy(db, step).start())
    land[0] = prod[pl.ds(flat * own, own)]
    pot_self.wait()
    for z in range(1, lines):
        pot_line(z).wait_recv()
    for p in range(1, near):
        pot_plane(p).start()
    for db in range(1, bands):
        pass_copy(0, db, band).start()

    for i in range(own):

        def scatter(z, carry, i=i):
            total = None
            for p in range(near):
                step = near * z + p
                values = None
                for db in range(bands):
                    if i == 0:
                        if db or p:
                            val_copy(db, step).wait_recv()
                        else:
                            pl.when(z > 0)(lambda: val_copy(0, step).wait_recv())
                    piece = land[db * groups + step, i]
                    values = piece if values is None else values + piece
                at = pl.ds(pl.multiple_of(peer(step) * slots, slots), slots)
                hits = cols_hot[:, at]
                placed = jnp.concatenate(
                    [hits * part[c : c + 1, :] for part in split_parts(values) for c in range(2)], axis=0
                )
                term = dot(rows_hot[:, at], placed, ((1,), (1,)))
                total = term if total is None else total + term
            grid[...] += total
            return carry

        grid[...] = jnp.zeros_like(grid)
        lax.fori_loop(0, lines, scatter, 0)
        if i == 0:
            for p in range(1, near):
                pot_plane(p).wait_recv()
                for db in range(1, bands):
                    pass_copy(p, db, band).start()

        def pot_ready():
            for p in range(near):
                for db in range(1, bands):
                    pass_copy(p, db, lax.rem(band + bands - db, bands)).wait_recv()

        apply_kernel(
            sz, i, pot_ready if i == 0 else None, grid, lambda ga: pot[pot_slot(ga)], pot.shape[2], groups, right,
            right_t, fore, back, twist, kin, space, out_ref
        )
    every(lambda db, step: val_copy(db, step).wait_send())
    for z in range(lines):
        for p in range(near):
            if z or p:
                rot_copy(z, p).wait_send()
    for z in range(1, lines):
        pot_line(z).wait_send()
    for p in range(1, near):
        pot_plane(p).wait_send()
    for p in range(near):
        for db in range(1, bands):
            pass_copy(p, db, band).wait_send()


def apply_kernel(
    sz, index, pot_ready, grid, pot_block, each, groups, right, right_t, fore, back, twist, kin, space, out_ref
):
    whole = 2 * sz.lanes
    summed = grid[:, :whole] + grid[:, whole:]
    field = jnp.concatenate(
        [
            summed[f * sz.rows : (f + 1) * sz.rows, c * sz.lanes : (c + 1) * sz.lanes]
            for c in range(2)
            for f in range(sz.fold)
        ],
        axis=1,
    )
    field_high, field_low = split_parts(field)
    step = 256
    for at in range(0, sz.wide, step):
        halves = []
        for c in range(2):
            here = slice(c * sz.wide + at, c * sz.wide + at + step)
            halves.append(
                dot(field_high, right[0, :, here])
                + (dot(field_low, right[0, :, here]) + dot(field_high, right[1, :, here]))
            )
        real = halves[0].reshape(sz.low, sz.window, step)
        imag = halves[1].reshape(sz.low, sz.window, step)
        cos = twist[0, :, at : at + step][:, None, :]
        sin = twist[1, :, at : at + step][:, None, :]
        turned = jnp.concatenate(
            [
                (real * cos - imag * sin).reshape(sz.rows, step),
                (real * sin + imag * cos).reshape(sz.rows, step),
            ],
            axis=0,
        )
        high, low = split_parts(turned)
        space[:, at : at + step] = dot(fore[0], high) + (dot(fore[0], low) + dot(fore[1], high))
    if pot_ready is not None:
        pot_ready()
    per = groups // sz.low
    applied = None
    for at in range(0, sz.wide, step):
        blocks = []
        for k_high in range(sz.low):
            lane = []
            for q in range(at // each, (at + step + each - 1) // each):
                lane.append(pot_block(k_high * per + q))
            blocks.append(lane[0] if len(lane) == 1 else jnp.concatenate(lane, axis=1))
        local = jnp.concatenate(blocks, axis=0)
        high, low = split_parts(space[:, at : at + step] * jnp.concatenate([local, local], axis=0))
        spread = dot(back[0], high) + (dot(back[0], low) + dot(back[1], high))
        real = spread[: sz.rows].reshape(sz.low, sz.window, step)
        imag = spread[sz.rows :].reshape(sz.low, sz.window, step)
        cos = twist[0, :, at : at + step][:, None, :]
        sin = twist[1, :, at : at + step][:, None, :]
        turned = [
            (real * cos + imag * sin).reshape(sz.rows, step),
            (imag * cos - real * sin).reshape(sz.rows, step),
        ]
        for c in range(2):
            here = slice(c * sz.wide + at, c * sz.wide + at + step)
            high, low = split_parts(turned[c])
            term = dot(high, right_t[0, here, :]) + (
                dot(low, right_t[0, here, :]) + dot(high, right_t[1, here, :])
            )
            applied = term if applied is None else applied + term
    applied = applied + jnp.concatenate([kin[...], kin[...]], axis=1) * field
    for c in range(2):
        pieces = [
            applied[lo * sz.window : (lo + 1) * sz.window, c * sz.cols + hi * sz.window : c * sz.cols + (hi + 1) * sz.window]
            for hi in range(sz.high)
            for lo in range(sz.low)
        ]
        out_ref[index, c] = jnp.concatenate(pieces, axis=1)


def run(coefficients, rotation, potential, index_map, counts, box):
    bands, groups = lax.axis_size("band"), lax.axis_size("ga")
    sz = Sizes(box, box // 2)
    depth, _, slots = coefficients.shape
    cols = rotation.shape[2]
    panel = cols * groups
    own = panel // (bands * groups)
    consts = [jnp.asarray(t) for t in tables(sz)]
    hbm = pl.BlockSpec(memory_space=pl.ANY)
    dma = pltpu.SemaphoreType.DMA
    return pl.pallas_call(
        functools.partial(whole_kernel, bands, groups, sz),
        out_shape=jax.ShapeDtypeStruct((own, 2, sz.window, sz.window * sz.window), F32),
        in_specs=[hbm] * 10,
        out_specs=pl.BlockSpec(memory_space=pltpu.VMEM),
        scratch_shapes=[
            pltpu.VMEM((2, depth, slots), F32),
            pltpu.VMEM((2, cols, depth), F32),
            pltpu.VMEM((1, index_map.shape[0]), I32),
            pltpu.SMEM(counts.shape, I32),
            *[pltpu.VMEM(table.shape, table.dtype) for table in consts],
            pltpu.VMEM((2, 2 * sz.cols, 2 * sz.wide), BF16),
            pltpu.VMEM((2, 2 * sz.wide, 2 * sz.cols), BF16),
            pltpu.VMEM((sz.fold * sz.rows, index_map.shape[0]), BF16),
            pltpu.VMEM((sz.lanes, index_map.shape[0]), BF16),
            pltpu.VMEM((2, 2 * depth, slots), BF16),
            pltpu.VMEM((groups, 2, cols, depth), F32),
            pltpu.VMEM((panel, 2, slots), F32),
            pltpu.VMEM((bands * groups, own, 2, slots), F32),
            pltpu.VMEM((groups,) + potential.shape, F32),
            pltpu.VMEM((sz.fold * sz.rows, 4 * sz.lanes), F32),
            pltpu.VMEM((2 * sz.deep, sz.wide), F32),
            pltpu.VMEM((sz.rows, sz.cols), F32),
            dma((10,)),
            dma((2,)),
            dma((groups,)),
            dma((groups,)),
            dma((groups,)),
            dma((groups,)),
            dma((bands, 4)),
            dma((bands, 4)),
            dma((bands * groups,)),
            dma((bands * groups,)),
        ],
        compiler_params=pltpu.CompilerParams(
            collective_id=0, has_side_effects=True, vmem_limit_bytes=60 * 1024 * 1024
        ),
    )(coefficients, rotation.transpose(0, 2, 1), potential, index_map[None], counts, *consts)


def per_device(coefficients, rotation, potential, index_map, counts):
    return run(coefficients, rotation, potential, index_map, counts, potential.shape[0])


def solution(mesh):
    placed = (P("band", None, "ga"), P(None, "band", "ga"), P(None, "ga"), P(), P())
    return jax.shard_map(
        per_device,
        mesh=mesh,
        in_specs=placed,
        out_specs=P(("band", "ga"), None, None, None),
        check_vma=False,
    )
```

```python
import functools
import math

import jax
import jax.numpy as jnp
import numpy as np
from jax import lax
from jax.experimental import pallas as pl
from jax.experimental.pallas import tpu as pltpu
from jax.sharding import PartitionSpec as P

F32 = jnp.float32
BF16 = jnp.bfloat16
I32 = jnp.int32
MESH = pl.DeviceIdType.MESH


def split_parts(values):
    high = values.astype(BF16)
    return high, (values - high.astype(F32)).astype(BF16)


def two_parts(table):
    high = table.astype(BF16)
    low = (table - high.astype(np.float32)).astype(BF16)
    return np.stack([high, low])


class Sizes:
    def __init__(self, box, window):
        self.box, self.window, self.half = box, window, window // 2
        self.low = 4
        self.high = window // self.low
        self.span = box // self.low
        self.rows = self.low * window
        self.cols = self.high * window
        self.wide = self.span * box
        self.deep = self.low * box
        self.fold = 2
        self.lanes = self.cols // self.fold
        assert box % self.low == 0 and box == 2 * window and box & (box - 1) == 0


def tables(sz):
    n_signed = np.arange(sz.window) - sz.half
    k_all = np.arange(sz.box)
    y_start = sz.low * np.arange(sz.high) - sz.half
    k_low = np.arange(sz.span)
    digit = np.arange(sz.low)

    def pair(phase):
        angle = (phase % sz.box) * (2.0 * math.pi / sz.box)
        return np.stack([np.cos(angle), np.sin(angle)])

    y_phase = y_start[:, None] * k_low[None, :]
    z_phase = n_signed[:, None] * k_all[None, :]
    base = np.concatenate(
        [pair(np.tile(z_phase, (1, sz.span))), pair(np.repeat(y_phase, sz.box, axis=1))], axis=1
    )
    flip = np.concatenate(
        [pair(np.tile(z_phase.T, (1, sz.high))), pair(np.repeat(y_phase.T, sz.window, axis=1))], axis=1
    )
    twist = pair(np.repeat(digit[:, None] * k_low[None, :], sz.box, axis=1))
    l_phase = sz.span * digit[:, None] * digit[None, :]
    x_phase = k_all[:, None] * n_signed[None, :]
    left = (l_phase[:, None, :, None] + x_phase[None, :, None, :]).reshape(sz.deep, sz.rows)
    cos, sin = pair(left)
    fore = two_parts((np.block([[cos, -sin], [sin, cos]]) / sz.box**3).astype(np.float32))
    back = two_parts(np.block([[cos.T, sin.T], [-sin.T, cos.T]]).astype(np.float32))
    return base.astype(np.float32), flip.astype(np.float32), twist.astype(np.float32), fore, back


def dot(a, b, dims=((1,), (0,))):
    return lax.dot_general(a, b, (dims, ((), ())), preferred_element_type=F32)


def whole_kernel(
    bands, groups, sz, coef_hbm, rot_hbm, pot_hbm, idx_hbm, cnt_hbm, base_hbm, flip_hbm, twist_hbm,
    fore_hbm, back_hbm, out_ref, coef, rot_ref, idx, cnt, base, flip, twist, fore, back, right, right_t,
    rows_hot, cols_hot, parts, rots, prod, land, pot, grid, space, kin, load_sem, self_sem, rot_send,
    rot_recv, pot_send, pot_recv, pass_send, pass_recv, val_send, val_recv
):
    band = lax.axis_index("band")
    me = lax.axis_index("ga")
    flat = band * groups + me
    depth, slots = coef.shape[1], coef.shape[2]
    cols = rot_ref.shape[1]
    panel = groups * cols
    own = land.shape[1]
    share_rows = pot_hbm.shape[0] // bands

    def share(holder):
        return pl.ds(pl.multiple_of(holder * share_rows, share_rows), share_rows)

    def load(src, dst, at):
        return pltpu.make_async_copy(src, dst, load_sem.at[at])

    rot_load = load(rot_hbm, rot_ref, 0)
    rot_load.start()
    small = [
        load(src, dst, at + 1)
        for at, (src, dst) in enumerate(
            (
                (base_hbm, base), (flip_hbm, flip), (idx_hbm, idx), (cnt_hbm, cnt), (twist_hbm, twist),
                (fore_hbm, fore), (back_hbm, back),
            )
        )
    ]
    coef_load = [load(coef_hbm.at[:, c, :], coef.at[c], 8 + c) for c in range(2)]
    for item in small[:4] + coef_load + small[4:]:
        item.start()

    near = 4 if groups % 4 == 0 else 1
    lines = groups // near
    assert groups & (groups - 1) == 0

    def flip_bits(value, mask, count):
        total, bit = 0, 1
        while bit < count:
            ours, theirs = lax.rem(value // bit, 2), lax.rem(mask // bit, 2) if not isinstance(mask, int) else mask // bit % 2
            total = total + bit * (ours + theirs - 2 * ours * theirs)
            bit *= 2
        return total

    def peer(step):
        return flip_bits(me, step, groups)

    barrier = pltpu.get_barrier_semaphore()
    hops = [(0, near * z) for z in range(1, lines)] + [(0, p) for p in range(1, near)]
    hops += [(db, 0) for db in range(1, bands)]

    def ahead(db, step):
        return {"band": lax.rem(band + db, bands), "ga": peer(step)}

    for db, step in hops:
        pl.semaphore_signal(barrier, inc=1, device_id=ahead(db, step), device_id_type=MESH)
    rot_load.wait()
    rot_self = pltpu.make_async_copy(rot_hbm, rots.at[me], self_sem.at[0])
    rot_self.start()
    pot_self = pltpu.make_async_copy(pot_hbm.at[share(band)], pot.at[0, share(band)], self_sem.at[1])
    pot_self.start()
    pl.semaphore_wait(barrier, len(hops))

    def rot_copy(z, p):
        slot = peer(near * z) if p else me
        return pltpu.make_async_remote_copy(
            src_ref=rots.at[slot] if z and p else rot_ref, dst_ref=rots.at[slot],
            send_sem=rot_send.at[near * z + p], recv_sem=rot_recv.at[near * z + p],
            device_id=ahead(0, p if p else near * z), device_id_type=MESH,
        )

    def pot_line(z):
        return pltpu.make_async_remote_copy(
            src_ref=pot_hbm.at[share(band)], dst_ref=pot.at[z, share(band)],
            send_sem=pot_send.at[z], recv_sem=pot_recv.at[z],
            device_id=ahead(0, near * z), device_id_type=MESH,
        )

    def pot_plane(p):
        return pltpu.make_async_remote_copy(
            src_ref=pot.at[pl.ds(0, lines), share(band)], dst_ref=pot.at[pl.ds(p * lines, lines), share(band)],
            send_sem=pot_send.at[lines + p], recv_sem=pot_recv.at[lines + p],
            device_id=ahead(0, p), device_id_type=MESH,
        )

    def pass_copy(p, db, holder):
        held = pot.at[pl.ds(p * lines, lines), share(holder)]
        return pltpu.make_async_remote_copy(
            src_ref=held, dst_ref=held, send_sem=pass_send.at[db, p], recv_sem=pass_recv.at[db, p],
            device_id=ahead(db, 0), device_id_type=MESH,
        )

    def val_copy(db, step):
        to = ahead(db, step)
        at = db * groups + step
        return pltpu.make_async_remote_copy(
            src_ref=prod.at[pl.ds((to["band"] * groups + to["ga"]) * own, own)], dst_ref=land.at[at],
            send_sem=val_send.at[at], recv_sem=val_recv.at[at], device_id=to, device_id_type=MESH,
        )

    def pot_slot(ga):
        step = peer(ga)
        return lax.rem(step, near) * lines + step // near

    def every(act):
        if bands * groups <= 64:
            for step in reversed(range(groups)):
                for db in range(bands):
                    if db or step:
                        act(db, step)
        else:

            def body(at, carry):
                act(at // groups, lax.rem(at, groups))
                return carry

            lax.fori_loop(1, bands * groups, body, 0)

    for z in range(1, lines):
        rot_copy(z, 0).start()
    for p in range(1, near):
        rot_copy(0, p).start()

    small[0].wait()

    def fill_right(step, carry):
        at = pl.multiple_of(step * sz.window, sz.window)
        y_cos = base[0, pl.ds(sz.window + step, 1), :]
        y_sin = base[1, pl.ds(sz.window + step, 1), :]
        z_cos, z_sin = base[0, : sz.window, :], base[1, : sz.window, :]
        cos = split_parts(z_cos * y_cos - z_sin * y_sin)
        sin = split_parts(z_sin * y_cos + z_cos * y_sin)
        for part in range(2):
            right[part, pl.ds(at, sz.window), : sz.wide] = cos[part]
            right[part, pl.ds(at, sz.window), sz.wide :] = sin[part]
            right[part, pl.ds(sz.cols + at, sz.window), : sz.wide] = -sin[part]
            right[part, pl.ds(sz.cols + at, sz.window), sz.wide :] = cos[part]
        return carry

    lax.fori_loop(0, sz.high, fill_right, 0)
    for z in range(1, lines):
        pot_line(z).start()
    small[1].wait()

    def fill_right_t(step, carry):
        at = pl.multiple_of(step * sz.box, sz.box)
        y_cos = flip[0, pl.ds(sz.box + step, 1), :]
        y_sin = flip[1, pl.ds(sz.box + step, 1), :]
        z_cos, z_sin = flip[0, : sz.box, :], flip[1, : sz.box, :]
        cos = split_parts(z_cos * y_cos - z_sin * y_sin)
        sin = split_parts(z_sin * y_cos + z_cos * y_sin)
        for part in range(2):
            right_t[part, pl.ds(at, sz.box), : sz.cols] = cos[part]
            right_t[part, pl.ds(at, sz.box), sz.cols :] = -sin[part]
            right_t[part, pl.ds(sz.wide + at, sz.box), : sz.cols] = sin[part]
            right_t[part, pl.ds(sz.wide + at, sz.box), sz.cols :] = cos[part]
        return carry

    lax.fori_loop(0, sz.span, fill_right_t, 0)
    for z in range(1, lines):
        rot_copy(z, 0).wait_recv()
        for p in range(1, near):
            rot_copy(z, p).start()
    small[2].wait()
    small[3].wait()
    bits = sz.box.bit_length() - 1

    def fill_hot(step, carry):
        at = pl.ds(pl.multiple_of(step * slots, slots), slots)
        cell = idx[:, at]
        n_x = (jnp.right_shift(cell, 2 * bits) + sz.half) & (sz.box - 1)
        n_y = (jnp.right_shift(cell, bits) + sz.half) & (sz.box - 1)
        n_z = (cell + sz.half) & (sz.box - 1)
        live = lax.broadcasted_iota(I32, (1, slots), 1) < cnt[step]
        live = live & (n_x < sz.window) & (n_y < sz.window) & (n_z < sz.window)
        y_high, y_low = n_y // sz.low, n_y % sz.low
        block, fine = y_high // (sz.high // sz.fold), y_high % (sz.high // sz.fold)
        row = jnp.where(live, block * sz.rows + y_low * sz.window + n_x, -1)
        col = fine * sz.window + n_z
        row_at = lax.broadcasted_iota(I32, (sz.fold * sz.rows, slots), 0)
        col_at = lax.broadcasted_iota(I32, (sz.lanes, slots), 0)
        rows_hot[:, at] = jnp.where(row_at == row, 1.0, 0.0).astype(BF16)
        cols_hot[:, at] = jnp.where(col_at == col, 1.0, 0.0).astype(BF16)
        return carry

    lax.fori_loop(0, groups, fill_hot, 0)
    row_at = lax.broadcasted_iota(I32, (sz.rows, sz.cols), 0)
    col_at = lax.broadcasted_iota(I32, (sz.rows, sz.cols), 1)
    n_x = (row_at % sz.window - sz.half).astype(F32)
    n_y = (col_at // sz.window * sz.low + row_at // sz.window - sz.half).astype(F32)
    n_z = (col_at % sz.window - sz.half).astype(F32)
    kin[...] = (8.0 / (sz.box * sz.box)) * (n_x * n_x + n_y * n_y + n_z * n_z)

    slab = 128
    for c in range(2):
        coef_load[c].wait()

        def fill_parts(step, carry, c=c):
            at = pl.multiple_of(step * slab, slab)
            high, low = split_parts(coef[c, pl.ds(at, slab), :])
            parts[0, pl.ds(c * depth + at, slab), :] = high
            parts[1, pl.ds(c * depth + at, slab), :] = low
            return carry

        lax.fori_loop(0, depth // slab, fill_parts, 0)
    for item in small[4:]:
        item.wait()

    rot_self.wait()
    for z in range(lines):
        for p in range(1, near):
            rot_copy(z, p).wait_recv()
    real = rots[:, 0].reshape(panel, depth)
    imag = rots[:, 1].reshape(panel, depth)
    mixer = jnp.concatenate(
        [jnp.concatenate([real, -imag], axis=1), jnp.concatenate([imag, real], axis=1)], axis=0
    )
    high, low = split_parts(mixer)
    first = dot(jnp.concatenate([high, low], axis=0), parts[0])
    mixed = first[: 2 * panel] + first[2 * panel :] + dot(high, parts[1])
    prod[:, 0, :] = mixed[:panel]
    prod[:, 1, :] = mixed[panel:]

    every(lambda db, step: val_copy(db, step).start())
    land[0] = prod[pl.ds(flat * own, own)]
    pot_self.wait()
    for z in range(1, lines):
        pot_line(z).wait_recv()
    for p in range(1, near):
        pot_plane(p).start()
    for db in range(1, bands):
        pass_copy(0, db, band).start()

    for i in range(own):

        def scatter(z, carry, i=i):
            total = None
            for p in range(near):
                step = near * z + p
                values = None
                for db in range(bands):
                    if i == 0:
                        if db or p:
                            val_copy(db, step).wait_recv()
                        else:
                            pl.when(z > 0)(lambda: val_copy(0, step).wait_recv())
                    piece = land[db * groups + step, i]
                    values = piece if values is None else values + piece
                at = pl.ds(pl.multiple_of(peer(step) * slots, slots), slots)
                hits = cols_hot[:, at]
                placed = jnp.concatenate(
                    [hits * part[c : c + 1, :] for part in split_parts(values) for c in range(2)], axis=0
                )
                term = dot(rows_hot[:, at], placed, ((1,), (1,)))
                total = term if total is None else total + term
            grid[...] += total
            return carry

        grid[...] = jnp.zeros_like(grid)
        lax.fori_loop(0, lines, scatter, 0)
        if i == 0:
            for p in range(1, near):
                pot_plane(p).wait_recv()
                for db in range(1, bands):
                    pass_copy(p, db, band).start()

        def pot_ready():
            for p in range(near):
                for db in range(1, bands):
                    pass_copy(p, db, lax.rem(band + bands - db, bands)).wait_recv()

        apply_kernel(
            sz, i, pot_ready if i == 0 else None, grid, lambda ga: pot[pot_slot(ga)], pot.shape[2], groups, right,
            right_t, fore, back, twist, kin, space, out_ref
        )
    every(lambda db, step: val_copy(db, step).wait_send())
    for z in range(lines):
        for p in range(near):
            if z or p:
                rot_copy(z, p).wait_send()
    for z in range(1, lines):
        pot_line(z).wait_send()
    for p in range(1, near):
        pot_plane(p).wait_send()
    for p in range(near):
        for db in range(1, bands):
            pass_copy(p, db, band).wait_send()


def apply_kernel(
    sz, index, pot_ready, grid, pot_block, each, groups, right, right_t, fore, back, twist, kin, space, out_ref
):
    whole = 2 * sz.lanes
    summed = grid[:, :whole] + grid[:, whole:]
    field = jnp.concatenate(
        [
            summed[f * sz.rows : (f + 1) * sz.rows, c * sz.lanes : (c + 1) * sz.lanes]
            for c in range(2)
            for f in range(sz.fold)
        ],
        axis=1,
    )
    field_high, field_low = split_parts(field)
    step = 256
    for at in range(0, sz.wide, step):
        halves = []
        for c in range(2):
            here = slice(c * sz.wide + at, c * sz.wide + at + step)
            halves.append(
                dot(field_high, right[0, :, here])
                + (dot(field_low, right[0, :, here]) + dot(field_high, right[1, :, here]))
            )
        real = halves[0].reshape(sz.low, sz.window, step)
        imag = halves[1].reshape(sz.low, sz.window, step)
        cos = twist[0, :, at : at + step][:, None, :]
        sin = twist[1, :, at : at + step][:, None, :]
        turned = jnp.concatenate(
            [
                (real * cos - imag * sin).reshape(sz.rows, step),
                (real * sin + imag * cos).reshape(sz.rows, step),
            ],
            axis=0,
        )
        high, low = split_parts(turned)
        space[:, at : at + step] = dot(fore[0], high) + (dot(fore[0], low) + dot(fore[1], high))
    if pot_ready is not None:
        pot_ready()
    per = groups // sz.low
    applied = None
    for at in range(0, sz.wide, step):
        blocks = []
        for k_high in range(sz.low):
            lane = []
            for q in range(at // each, (at + step + each - 1) // each):
                lane.append(pot_block(k_high * per + q))
            blocks.append(lane[0] if len(lane) == 1 else jnp.concatenate(lane, axis=1))
        local = jnp.concatenate(blocks, axis=0)
        high, low = split_parts(space[:, at : at + step] * jnp.concatenate([local, local], axis=0))
        spread = dot(back[0], high) + (dot(back[0], low) + dot(back[1], high))
        real = spread[: sz.rows].reshape(sz.low, sz.window, step)
        imag = spread[sz.rows :].reshape(sz.low, sz.window, step)
        cos = twist[0, :, at : at + step][:, None, :]
        sin = twist[1, :, at : at + step][:, None, :]
        turned = [
            (real * cos + imag * sin).reshape(sz.rows, step),
            (imag * cos - real * sin).reshape(sz.rows, step),
        ]
        for c in range(2):
            here = slice(c * sz.wide + at, c * sz.wide + at + step)
            high, low = split_parts(turned[c])
            term = dot(high, right_t[0, here, :]) + (
                dot(low, right_t[0, here, :]) + dot(high, right_t[1, here, :])
            )
            applied = term if applied is None else applied + term
    applied = applied + jnp.concatenate([kin[...], kin[...]], axis=1) * field
    for c in range(2):
        pieces = [
            applied[lo * sz.window : (lo + 1) * sz.window, c * sz.cols + hi * sz.window : c * sz.cols + (hi + 1) * sz.window]
            for hi in range(sz.high)
            for lo in range(sz.low)
        ]
        out_ref[index, c] = jnp.concatenate(pieces, axis=1)


def run(coefficients, rotation, potential, index_map, counts, box):
    bands, groups = lax.axis_size("band"), lax.axis_size("ga")
    sz = Sizes(box, box // 2)
    depth, _, slots = coefficients.shape
    cols = rotation.shape[2]
    panel = cols * groups
    own = panel // (bands * groups)
    consts = [jnp.asarray(t) for t in tables(sz)]
    hbm = pl.BlockSpec(memory_space=pl.ANY)
    dma = pltpu.SemaphoreType.DMA
    return pl.pallas_call(
        functools.partial(whole_kernel, bands, groups, sz),
        out_shape=pltpu.VMEM((own, 2, sz.window, sz.window * sz.window), F32),
        in_specs=[hbm] * 10,
        out_specs=pl.BlockSpec(memory_space=pltpu.VMEM),
        scratch_shapes=[
            pltpu.VMEM((2, depth, slots), F32),
            pltpu.VMEM((2, cols, depth), F32),
            pltpu.VMEM((1, index_map.shape[0]), I32),
            pltpu.SMEM(counts.shape, I32),
            *[pltpu.VMEM(table.shape, table.dtype) for table in consts],
            pltpu.VMEM((2, 2 * sz.cols, 2 * sz.wide), BF16),
            pltpu.VMEM((2, 2 * sz.wide, 2 * sz.cols), BF16),
            pltpu.VMEM((sz.fold * sz.rows, index_map.shape[0]), BF16),
            pltpu.VMEM((sz.lanes, index_map.shape[0]), BF16),
            pltpu.VMEM((2, 2 * depth, slots), BF16),
            pltpu.VMEM((groups, 2, cols, depth), F32),
            pltpu.VMEM((panel, 2, slots), F32),
            pltpu.VMEM((bands * groups, own, 2, slots), F32),
            pltpu.VMEM((groups,) + potential.shape, F32),
            pltpu.VMEM((sz.fold * sz.rows, 4 * sz.lanes), F32),
            pltpu.VMEM((2 * sz.deep, sz.wide), F32),
            pltpu.VMEM((sz.rows, sz.cols), F32),
            dma((10,)),
            dma((2,)),
            dma((groups,)),
            dma((groups,)),
            dma((groups,)),
            dma((groups,)),
            dma((bands, 4)),
            dma((bands, 4)),
            dma((bands * groups,)),
            dma((bands * groups,)),
        ],
        compiler_params=pltpu.CompilerParams(
            collective_id=0, has_side_effects=True, vmem_limit_bytes=60 * 1024 * 1024
        ),
    )(coefficients, rotation.transpose(0, 2, 1), potential, index_map[None], counts, *consts)


def per_device(coefficients, rotation, potential, index_map, counts):
    return run(coefficients, rotation, potential, index_map, counts, potential.shape[0])


def solution(mesh):
    placed = (P("band", None, "ga"), P(None, "band", "ga"), P(None, "ga"), P(), P())
    return jax.shard_map(
        per_device,
        mesh=mesh,
        in_specs=placed,
        out_specs=P(("band", "ga"), None, None, None),
        check_vma=False,
    )
```

```python
import functools
import math

import jax
import jax.numpy as jnp
import numpy as np
from jax import lax
from jax.experimental import pallas as pl
from jax.experimental.pallas import tpu as pltpu
from jax.sharding import PartitionSpec as P

F32 = jnp.float32
BF16 = jnp.bfloat16
I32 = jnp.int32
MESH = pl.DeviceIdType.MESH


def split_parts(values):
    high = values.astype(BF16)
    return high, (values - high.astype(F32)).astype(BF16)


def two_parts(table):
    high = table.astype(BF16)
    low = (table - high.astype(np.float32)).astype(BF16)
    return np.stack([high, low])


class Sizes:
    def __init__(self, box, window):
        self.box, self.window, self.half = box, window, window // 2
        self.low = 4
        self.high = window // self.low
        self.span = box // self.low
        self.rows = self.low * window
        self.cols = self.high * window
        self.wide = self.span * box
        self.deep = self.low * box
        self.fold = 2
        self.lanes = self.cols // self.fold
        assert box % self.low == 0 and box == 2 * window and box & (box - 1) == 0


def tables(sz):
    n_signed = np.arange(sz.window) - sz.half
    k_all = np.arange(sz.box)
    y_start = sz.low * np.arange(sz.high) - sz.half
    k_low = np.arange(sz.span)
    digit = np.arange(sz.low)

    def pair(phase):
        angle = (phase % sz.box) * (2.0 * math.pi / sz.box)
        return np.stack([np.cos(angle), np.sin(angle)])

    y_phase = y_start[:, None] * k_low[None, :]
    z_phase = n_signed[:, None] * k_all[None, :]
    base = np.concatenate(
        [pair(np.tile(z_phase, (1, sz.span))), pair(np.repeat(y_phase, sz.box, axis=1))], axis=1
    )
    flip = np.concatenate(
        [pair(np.tile(z_phase.T, (1, sz.high))), pair(np.repeat(y_phase.T, sz.window, axis=1))], axis=1
    )
    twist = pair(np.repeat(digit[:, None] * k_low[None, :], sz.box, axis=1))
    cos, sin = pair(k_all[:, None] * n_signed[None, :])

    def three(table):
        high, low = two_parts(table.astype(np.float32))
        return np.concatenate([high, high, low], axis=1)

    fore = three(np.block([[cos, -sin], [sin, cos]]) / sz.box**3)
    back = three(np.block([[cos.T, sin.T], [-sin.T, cos.T]]))
    return base.astype(np.float32), flip.astype(np.float32), twist.astype(np.float32), fore, back


def dot(a, b, dims=((1,), (0,))):
    return lax.dot_general(a, b, (dims, ((), ())), preferred_element_type=F32)


def whole_kernel(
    bands, groups, sz, coef_hbm, rot_hbm, pot_hbm, idx_hbm, cnt_hbm, base_hbm, flip_hbm, twist_hbm,
    fore_hbm, back_hbm, out_ref, coef, rot_ref, idx, cnt, base, flip, twist, fore, back, right, right_t,
    rows_hot, cols_hot, parts, rots, prod, land, pot, grid, space, kin, load_sem, self_sem, rot_send,
    rot_recv, pot_send, pot_recv, pass_send, pass_recv, val_send, val_recv
):
    band = lax.axis_index("band")
    me = lax.axis_index("ga")
    flat = band * groups + me
    depth, slots = coef.shape[1], coef.shape[2]
    cols = rot_ref.shape[1]
    panel = groups * cols
    own = land.shape[1]
    share_rows = pot_hbm.shape[0] // bands

    def share(holder):
        return pl.ds(pl.multiple_of(holder * share_rows, share_rows), share_rows)

    def load(src, dst, at):
        return pltpu.make_async_copy(src, dst, load_sem.at[at])

    rot_load = load(rot_hbm, rot_ref, 0)
    rot_load.start()
    small = [
        load(src, dst, at + 1)
        for at, (src, dst) in enumerate(
            (
                (base_hbm, base), (flip_hbm, flip), (idx_hbm, idx), (cnt_hbm, cnt), (twist_hbm, twist),
                (fore_hbm, fore), (back_hbm, back),
            )
        )
    ]
    coef_load = [load(coef_hbm.at[:, c, :], coef.at[c], 8 + c) for c in range(2)]
    for item in small[:4] + coef_load + small[4:]:
        item.start()

    near = 4 if groups % 4 == 0 else 1
    lines = groups // near
    assert groups & (groups - 1) == 0

    def flip_bits(value, mask, count):
        total, bit = 0, 1
        while bit < count:
            ours, theirs = lax.rem(value // bit, 2), lax.rem(mask // bit, 2) if not isinstance(mask, int) else mask // bit % 2
            total = total + bit * (ours + theirs - 2 * ours * theirs)
            bit *= 2
        return total

    def peer(step):
        return flip_bits(me, step, groups)

    barrier = pltpu.get_barrier_semaphore()
    hops = [(0, near * z) for z in range(1, lines)] + [(0, p) for p in range(1, near)]
    hops += [(db, 0) for db in range(1, bands)]

    def ahead(db, step):
        return {"band": lax.rem(band + db, bands), "ga": peer(step)}

    for db, step in hops:
        pl.semaphore_signal(barrier, inc=1, device_id=ahead(db, step), device_id_type=MESH)
    rot_load.wait()
    rot_self = pltpu.make_async_copy(rot_hbm, rots.at[me], self_sem.at[0])
    rot_self.start()
    pot_self = pltpu.make_async_copy(pot_hbm.at[share(band)], pot.at[0, share(band)], self_sem.at[1])
    pot_self.start()
    pl.semaphore_wait(barrier, len(hops))

    def rot_copy(z, p):
        slot = peer(near * z) if p else me
        return pltpu.make_async_remote_copy(
            src_ref=rots.at[slot] if z and p else rot_ref, dst_ref=rots.at[slot],
            send_sem=rot_send.at[near * z + p], recv_sem=rot_recv.at[near * z + p],
            device_id=ahead(0, p if p else near * z), device_id_type=MESH,
        )

    def pot_line(z):
        return pltpu.make_async_remote_copy(
            src_ref=pot_hbm.at[share(band)], dst_ref=pot.at[z, share(band)],
            send_sem=pot_send.at[z], recv_sem=pot_recv.at[z],
            device_id=ahead(0, near * z), device_id_type=MESH,
        )

    def pot_plane(p):
        return pltpu.make_async_remote_copy(
            src_ref=pot.at[pl.ds(0, lines), share(band)], dst_ref=pot.at[pl.ds(p * lines, lines), share(band)],
            send_sem=pot_send.at[lines + p], recv_sem=pot_recv.at[lines + p],
            device_id=ahead(0, p), device_id_type=MESH,
        )

    def pass_copy(p, db, holder):
        held = pot.at[pl.ds(p * lines, lines), share(holder)]
        return pltpu.make_async_remote_copy(
            src_ref=held, dst_ref=held, send_sem=pass_send.at[db, p], recv_sem=pass_recv.at[db, p],
            device_id=ahead(db, 0), device_id_type=MESH,
        )

    def val_copy(db, step):
        to = ahead(db, step)
        at = db * groups + step
        return pltpu.make_async_remote_copy(
            src_ref=prod.at[pl.ds((to["band"] * groups + to["ga"]) * own, own)], dst_ref=land.at[at],
            send_sem=val_send.at[at], recv_sem=val_recv.at[at], device_id=to, device_id_type=MESH,
        )

    def pot_slot(ga):
        step = peer(ga)
        return lax.rem(step, near) * lines + step // near

    def every(act):
        if bands * groups <= 64:
            for step in reversed(range(groups)):
                for db in range(bands):
                    if db or step:
                        act(db, step)
        else:

            def body(at, carry):
                act(at // groups, lax.rem(at, groups))
                return carry

            lax.fori_loop(1, bands * groups, body, 0)

    for z in range(1, lines):
        rot_copy(z, 0).start()
    for p in range(1, near):
        rot_copy(0, p).start()

    small[0].wait()

    def fill_right(step, carry):
        at = pl.multiple_of(step * sz.window, sz.window)
        y_cos = base[0, pl.ds(sz.window + step, 1), :]
        y_sin = base[1, pl.ds(sz.window + step, 1), :]
        z_cos, z_sin = base[0, : sz.window, :], base[1, : sz.window, :]
        cos = split_parts(z_cos * y_cos - z_sin * y_sin)
        sin = split_parts(z_sin * y_cos + z_cos * y_sin)
        for part in range(2):
            right[part, pl.ds(at, sz.window), : sz.wide] = cos[part]
            right[part, pl.ds(at, sz.window), sz.wide :] = sin[part]
            right[part, pl.ds(sz.cols + at, sz.window), : sz.wide] = -sin[part]
            right[part, pl.ds(sz.cols + at, sz.window), sz.wide :] = cos[part]
        return carry

    lax.fori_loop(0, sz.high, fill_right, 0)
    for z in range(1, lines):
        pot_line(z).start()
    small[1].wait()

    def fill_right_t(step, carry):
        at = pl.multiple_of(step * sz.box, sz.box)
        y_cos = flip[0, pl.ds(sz.box + step, 1), :]
        y_sin = flip[1, pl.ds(sz.box + step, 1), :]
        z_cos, z_sin = flip[0, : sz.box, :], flip[1, : sz.box, :]
        cos = split_parts(z_cos * y_cos - z_sin * y_sin)
        sin = split_parts(z_sin * y_cos + z_cos * y_sin)
        for part in range(2):
            right_t[part, pl.ds(at, sz.box), : sz.cols] = cos[part]
            right_t[part, pl.ds(at, sz.box), sz.cols :] = -sin[part]
            right_t[part, pl.ds(sz.wide + at, sz.box), : sz.cols] = sin[part]
            right_t[part, pl.ds(sz.wide + at, sz.box), sz.cols :] = cos[part]
        return carry

    lax.fori_loop(0, sz.span, fill_right_t, 0)
    for z in range(1, lines):
        rot_copy(z, 0).wait_recv()
        for p in range(1, near):
            rot_copy(z, p).start()
    small[2].wait()
    small[3].wait()
    bits = sz.box.bit_length() - 1

    def fill_hot(step, carry):
        at = pl.ds(pl.multiple_of(step * slots, slots), slots)
        cell = idx[:, at]
        n_x = (jnp.right_shift(cell, 2 * bits) + sz.half) & (sz.box - 1)
        n_y = (jnp.right_shift(cell, bits) + sz.half) & (sz.box - 1)
        n_z = (cell + sz.half) & (sz.box - 1)
        live = lax.broadcasted_iota(I32, (1, slots), 1) < cnt[step]
        live = live & (n_x < sz.window) & (n_y < sz.window) & (n_z < sz.window)
        y_high, y_low = n_y // sz.low, n_y % sz.low
        block, fine = y_high // (sz.high // sz.fold), y_high % (sz.high // sz.fold)
        row = jnp.where(live, block * sz.rows + y_low * sz.window + n_x, -1)
        col = fine * sz.window + n_z
        row_at = lax.broadcasted_iota(I32, (sz.fold * sz.rows, slots), 0)
        col_at = lax.broadcasted_iota(I32, (sz.lanes, slots), 0)
        rows_hot[:, at] = jnp.where(row_at == row, 1.0, 0.0).astype(BF16)
        cols_hot[:, at] = jnp.where(col_at == col, 1.0, 0.0).astype(BF16)
        return carry

    lax.fori_loop(0, groups, fill_hot, 0)
    row_at = lax.broadcasted_iota(I32, (sz.rows, sz.cols), 0)
    col_at = lax.broadcasted_iota(I32, (sz.rows, sz.cols), 1)
    n_x = (row_at % sz.window - sz.half).astype(F32)
    n_y = (col_at // sz.window * sz.low + row_at // sz.window - sz.half).astype(F32)
    n_z = (col_at % sz.window - sz.half).astype(F32)
    kin[...] = (8.0 / (sz.box * sz.box)) * (n_x * n_x + n_y * n_y + n_z * n_z)

    slab = 128
    for c in range(2):
        coef_load[c].wait()

        def fill_parts(step, carry, c=c):
            at = pl.multiple_of(step * slab, slab)
            high, low = split_parts(coef[c, pl.ds(at, slab), :])
            parts[0, pl.ds(c * depth + at, slab), :] = high
            parts[1, pl.ds(c * depth + at, slab), :] = low
            return carry

        lax.fori_loop(0, depth // slab, fill_parts, 0)
    for item in small[4:]:
        item.wait()

    rot_self.wait()
    for z in range(lines):
        for p in range(1, near):
            rot_copy(z, p).wait_recv()
    real = rots[:, 0].reshape(panel, depth)
    imag = rots[:, 1].reshape(panel, depth)
    mixer = jnp.concatenate(
        [jnp.concatenate([real, -imag], axis=1), jnp.concatenate([imag, real], axis=1)], axis=0
    )
    high, low = split_parts(mixer)
    first = dot(jnp.concatenate([high, low], axis=0), parts[0])
    mixed = first[: 2 * panel] + first[2 * panel :] + dot(high, parts[1])
    prod[:, 0, :] = mixed[:panel]
    prod[:, 1, :] = mixed[panel:]

    every(lambda db, step: val_copy(db, step).start())
    land[0] = prod[pl.ds(flat * own, own)]
    pot_self.wait()
    for z in range(1, lines):
        pot_line(z).wait_recv()
    for p in range(1, near):
        pot_plane(p).start()
    for db in range(1, bands):
        pass_copy(0, db, band).start()

    def relay(pieces):
        for p in pieces:
            pot_plane(p).wait_recv()
            for db in range(1, bands):
                pass_copy(p, db, band).start()

    for i in range(own):

        def scatter(z, carry, i=i):
            total = None
            for p in range(near):
                step = near * z + p
                values = None
                for db in range(bands):
                    if i == 0:
                        if db or p:
                            val_copy(db, step).wait_recv()
                        else:
                            pl.when(z > 0)(lambda: val_copy(0, step).wait_recv())
                    piece = land[db * groups + step, i]
                    values = piece if values is None else values + piece
                at = pl.ds(pl.multiple_of(peer(step) * slots, slots), slots)
                hits = cols_hot[:, at]
                placed = jnp.concatenate(
                    [hits * part[c : c + 1, :] for part in split_parts(values) for c in range(2)], axis=0
                )
                term = dot(rows_hot[:, at], placed, ((1,), (1,)))
                total = term if total is None else total + term
            grid[...] += total
            return carry

        grid[...] = jnp.zeros_like(grid)
        lax.fori_loop(0, lines, scatter, 0)
        if i == 0:
            relay(range(1, near))

        def pot_ready():
            for p in range(near):
                for db in range(1, bands):
                    pass_copy(p, db, lax.rem(band + bands - db, bands)).wait_recv()

        apply_kernel(
            sz, i, pot_ready if i == 0 else None, grid, lambda ga: pot[pot_slot(ga)], pot.shape[2], groups, right,
            right_t, fore, back, twist, kin, space, out_ref
        )
    every(lambda db, step: val_copy(db, step).wait_send())
    for z in range(lines):
        for p in range(near):
            if z or p:
                rot_copy(z, p).wait_send()
    for z in range(1, lines):
        pot_line(z).wait_send()
    for p in range(1, near):
        pot_plane(p).wait_send()
    for p in range(near):
        for db in range(1, bands):
            pass_copy(p, db, band).wait_send()


def quarter(real, imag, sign):
    even_r, even_i = real[0] + real[2], imag[0] + imag[2]
    odd_r, odd_i = real[0] - real[2], imag[0] - imag[2]
    both_r, both_i = real[1] + real[3], imag[1] + imag[3]
    gap_r, gap_i = sign * (real[1] - real[3]), sign * (imag[1] - imag[3])
    return (
        (even_r + both_r, even_i + both_i),
        (odd_r - gap_i, odd_i + gap_r),
        (even_r - both_r, even_i - both_i),
        (odd_r + gap_i, odd_i - gap_r),
    )


def apply_kernel(
    sz, index, pot_ready, grid, pot_block, each, groups, right, right_t, fore, back, twist, kin, space, out_ref
):
    whole = 2 * sz.lanes
    summed = grid[:, :whole] + grid[:, whole:]
    field = jnp.concatenate(
        [
            summed[f * sz.rows : (f + 1) * sz.rows, c * sz.lanes : (c + 1) * sz.lanes]
            for c in range(2)
            for f in range(sz.fold)
        ],
        axis=1,
    )
    field_high, field_low = split_parts(field)
    step = 256
    for at in range(0, sz.wide, step):
        halves = []
        for c in range(2):
            here = slice(c * sz.wide + at, c * sz.wide + at + step)
            halves.append(
                dot(field_high, right[0, :, here])
                + (dot(field_low, right[0, :, here]) + dot(field_high, right[1, :, here]))
            )
        real, imag = [], []
        for l in range(sz.low):
            cos, sin = twist[0, l : l + 1, at : at + step], twist[1, l : l + 1, at : at + step]
            a, b = [half[l * sz.window : (l + 1) * sz.window] for half in halves]
            real.append(a * cos - b * sin)
            imag.append(a * sin + b * cos)
        for k, (a, b) in enumerate(quarter(real, imag, 1)):
            high, low = split_parts(jnp.concatenate([a, b], axis=0))
            stacked = jnp.concatenate([high, low, high], axis=0)
            space[k * 2 * sz.box : (k + 1) * 2 * sz.box, at : at + step] = dot(fore[...], stacked)
    if pot_ready is not None:
        pot_ready()
    per = groups // sz.low
    applied = None
    for at in range(0, sz.wide, step):
        real, imag = [], []
        for k in range(sz.low):
            lane = [pot_block(k * per + q) for q in range(at // each, (at + step + each - 1) // each)]
            local = lane[0] if len(lane) == 1 else jnp.concatenate(lane, axis=1)
            here = space[k * 2 * sz.box : (k + 1) * 2 * sz.box, at : at + step]
            high, low = split_parts(here * jnp.concatenate([local, local], axis=0))
            spread = dot(back[...], jnp.concatenate([high, low, high], axis=0))
            real.append(spread[: sz.window])
            imag.append(spread[sz.window :])
        turned = [[], []]
        for l, (a, b) in enumerate(quarter(real, imag, -1)):
            cos, sin = twist[0, l : l + 1, at : at + step], twist[1, l : l + 1, at : at + step]
            turned[0].append(a * cos + b * sin)
            turned[1].append(b * cos - a * sin)
        turned = [jnp.concatenate(rows, axis=0) for rows in turned]
        for c in range(2):
            here = slice(c * sz.wide + at, c * sz.wide + at + step)
            high, low = split_parts(turned[c])
            term = dot(high, right_t[0, here, :]) + (
                dot(low, right_t[0, here, :]) + dot(high, right_t[1, here, :])
            )
            applied = term if applied is None else applied + term
    applied = applied + jnp.concatenate([kin[...], kin[...]], axis=1) * field
    for c in range(2):
        pieces = [
            applied[lo * sz.window : (lo + 1) * sz.window, c * sz.cols + hi * sz.window : c * sz.cols + (hi + 1) * sz.window]
            for hi in range(sz.high)
            for lo in range(sz.low)
        ]
        out_ref[index, c] = jnp.concatenate(pieces, axis=1)


def run(coefficients, rotation, potential, index_map, counts, box):
    bands, groups = lax.axis_size("band"), lax.axis_size("ga")
    sz = Sizes(box, box // 2)
    depth, _, slots = coefficients.shape
    cols = rotation.shape[2]
    panel = cols * groups
    own = panel // (bands * groups)
    consts = [jnp.asarray(t) for t in tables(sz)]
    hbm = pl.BlockSpec(memory_space=pl.ANY)
    dma = pltpu.SemaphoreType.DMA
    return pl.pallas_call(
        functools.partial(whole_kernel, bands, groups, sz),
        out_shape=pltpu.VMEM((own, 2, sz.window, sz.window * sz.window), F32),
        in_specs=[hbm] * 10,
        out_specs=pl.BlockSpec(memory_space=pltpu.VMEM),
        scratch_shapes=[
            pltpu.VMEM((2, depth, slots), F32),
            pltpu.VMEM((2, cols, depth), F32),
            pltpu.VMEM((1, index_map.shape[0]), I32),
            pltpu.SMEM(counts.shape, I32),
            *[pltpu.VMEM(table.shape, table.dtype) for table in consts],
            pltpu.VMEM((2, 2 * sz.cols, 2 * sz.wide), BF16),
            pltpu.VMEM((2, 2 * sz.wide, 2 * sz.cols), BF16),
            pltpu.VMEM((sz.fold * sz.rows, index_map.shape[0]), BF16),
            pltpu.VMEM((sz.lanes, index_map.shape[0]), BF16),
            pltpu.VMEM((2, 2 * depth, slots), BF16),
            pltpu.VMEM((groups, 2, cols, depth), F32),
            pltpu.VMEM((panel, 2, slots), F32),
            pltpu.VMEM((bands * groups, own, 2, slots), F32),
            pltpu.VMEM((groups,) + potential.shape, F32),
            pltpu.VMEM((sz.fold * sz.rows, 4 * sz.lanes), F32),
            pltpu.VMEM((2 * sz.deep, sz.wide), F32),
            pltpu.VMEM((sz.rows, sz.cols), F32),
            dma((10,)),
            dma((2,)),
            dma((groups,)),
            dma((groups,)),
            dma((groups,)),
            dma((groups,)),
            dma((bands, 4)),
            dma((bands, 4)),
            dma((bands * groups,)),
            dma((bands * groups,)),
        ],
        compiler_params=pltpu.CompilerParams(
            collective_id=0, has_side_effects=True, vmem_limit_bytes=60 * 1024 * 1024
        ),
    )(coefficients, rotation.transpose(0, 2, 1), potential, index_map[None], counts, *consts)


def per_device(coefficients, rotation, potential, index_map, counts):
    return run(coefficients, rotation, potential, index_map, counts, potential.shape[0])


def solution(mesh):
    placed = (P("band", None, "ga"), P(None, "band", "ga"), P(None, "ga"), P(), P())
    return jax.shard_map(
        per_device,
        mesh=mesh,
        in_specs=placed,
        out_specs=P(("band", "ga"), None, None, None),
        check_vma=False,
    )
```

```python
import functools
import math

import jax
import jax.numpy as jnp
import numpy as np
from jax import lax
from jax.experimental import pallas as pl
from jax.experimental.pallas import tpu as pltpu
from jax.sharding import PartitionSpec as P

F32 = jnp.float32
BF16 = jnp.bfloat16
I32 = jnp.int32
MESH = pl.DeviceIdType.MESH


def split_parts(values):
    high = values.astype(BF16)
    return high, (values - high.astype(F32)).astype(BF16)


def two_parts(table):
    high = table.astype(BF16)
    low = (table - high.astype(np.float32)).astype(BF16)
    return np.stack([high, low])


class Sizes:
    def __init__(self, box, window):
        self.box, self.window, self.half = box, window, window // 2
        self.low = 4
        self.high = window // self.low
        self.span = box // self.low
        self.rows = self.low * window
        self.cols = self.high * window
        self.wide = self.span * box
        self.deep = self.low * box
        self.fold = 2
        self.lanes = self.cols // self.fold
        assert box % self.low == 0 and box == 2 * window and box & (box - 1) == 0


def tables(sz):
    n_signed = np.arange(sz.window) - sz.half
    k_all = np.arange(sz.box)
    y_start = sz.low * np.arange(sz.high) - sz.half
    k_low = np.arange(sz.span)
    digit = np.arange(sz.low)

    def pair(phase):
        angle = (phase % sz.box) * (2.0 * math.pi / sz.box)
        return np.stack([np.cos(angle), np.sin(angle)])

    y_phase = y_start[:, None] * k_low[None, :]
    z_phase = n_signed[:, None] * k_all[None, :]
    base = np.concatenate(
        [pair(np.tile(z_phase, (1, sz.span))), pair(np.repeat(y_phase, sz.box, axis=1))], axis=1
    )
    flip = np.concatenate(
        [pair(np.tile(z_phase.T, (1, sz.high))), pair(np.repeat(y_phase.T, sz.window, axis=1))], axis=1
    )
    twist = pair(np.repeat(digit[:, None] * k_low[None, :], sz.box, axis=1))
    cos, sin = pair(k_all[:, None] * n_signed[None, :])

    def three(table):
        high, low = two_parts(table.astype(np.float32))
        return np.concatenate([high, high, low], axis=1)

    fore = three(np.block([[cos, -sin], [sin, cos]]) / sz.box**3)
    back = three(np.block([[cos.T, sin.T], [-sin.T, cos.T]]))
    return base.astype(np.float32), flip.astype(np.float32), twist.astype(np.float32), fore, back


def dot(a, b, dims=((1,), (0,))):
    return lax.dot_general(a, b, (dims, ((), ())), preferred_element_type=F32)


def whole_kernel(
    bands, groups, sz, coef_hbm, rot_hbm, pot_hbm, idx_hbm, cnt_hbm, base_hbm, flip_hbm, twist_hbm,
    fore_hbm, back_hbm, out_ref, coef, rot_ref, idx, cnt, base, flip, twist, fore, back, right, right_t,
    rows_hot, cols_hot, parts, rots, prod, land, pot, grid, space, kin, load_sem, self_sem, rot_send,
    rot_recv, pot_send, pot_recv, pass_send, pass_recv, val_send, val_recv
):
    band = lax.axis_index("band")
    me = lax.axis_index("ga")
    flat = band * groups + me
    depth, slots = coef.shape[1], coef.shape[2]
    cols = rot_ref.shape[1]
    panel = groups * cols
    own = land.shape[1]
    share_rows = pot_hbm.shape[0] // bands

    def share(holder):
        return pl.ds(pl.multiple_of(holder * share_rows, share_rows), share_rows)

    def load(src, dst, at):
        return pltpu.make_async_copy(src, dst, load_sem.at[at])

    rot_load = load(rot_hbm, rot_ref, 0)
    rot_load.start()
    small = [
        load(src, dst, at + 1)
        for at, (src, dst) in enumerate(
            (
                (base_hbm, base), (flip_hbm, flip), (idx_hbm, idx), (cnt_hbm, cnt), (twist_hbm, twist),
                (fore_hbm, fore), (back_hbm, back),
            )
        )
    ]
    coef_load = [load(coef_hbm.at[:, c, :], coef.at[c], 8 + c) for c in range(2)]
    for item in small[:4] + coef_load + small[4:]:
        item.start()

    near = 4 if groups % 4 == 0 else 1
    lines = groups // near
    assert groups & (groups - 1) == 0

    def flip_bits(value, mask, count):
        total, bit = 0, 1
        while bit < count:
            ours, theirs = lax.rem(value // bit, 2), lax.rem(mask // bit, 2) if not isinstance(mask, int) else mask // bit % 2
            total = total + bit * (ours + theirs - 2 * ours * theirs)
            bit *= 2
        return total

    def peer(step):
        return flip_bits(me, step, groups)

    barrier = pltpu.get_barrier_semaphore()
    hops = [(0, near * z) for z in range(1, lines)] + [(0, p) for p in range(1, near)]
    hops += [(db, 0) for db in range(1, bands)]

    def ahead(db, step):
        return {"band": lax.rem(band + db, bands), "ga": peer(step)}

    for db, step in hops:
        pl.semaphore_signal(barrier, inc=1, device_id=ahead(db, step), device_id_type=MESH)
    rot_load.wait()
    rot_self = pltpu.make_async_copy(rot_hbm, rots.at[me], self_sem.at[0])
    rot_self.start()
    pot_self = pltpu.make_async_copy(pot_hbm.at[share(band)], pot.at[0, share(band)], self_sem.at[1])
    pot_self.start()
    pl.semaphore_wait(barrier, len(hops))

    def rot_copy(z, p):
        slot = peer(near * z) if p else me
        return pltpu.make_async_remote_copy(
            src_ref=rots.at[slot] if z and p else rot_ref, dst_ref=rots.at[slot],
            send_sem=rot_send.at[near * z + p], recv_sem=rot_recv.at[near * z + p],
            device_id=ahead(0, p if p else near * z), device_id_type=MESH,
        )

    def pot_line(z):
        return pltpu.make_async_remote_copy(
            src_ref=pot_hbm.at[share(band)], dst_ref=pot.at[z, share(band)],
            send_sem=pot_send.at[z], recv_sem=pot_recv.at[z],
            device_id=ahead(0, near * z), device_id_type=MESH,
        )

    def pot_plane(p):
        return pltpu.make_async_remote_copy(
            src_ref=pot.at[pl.ds(0, lines), share(band)], dst_ref=pot.at[pl.ds(p * lines, lines), share(band)],
            send_sem=pot_send.at[lines + p], recv_sem=pot_recv.at[lines + p],
            device_id=ahead(0, p), device_id_type=MESH,
        )

    def pass_copy(p, db, holder):
        held = pot.at[pl.ds(p * lines, lines), share(holder)]
        return pltpu.make_async_remote_copy(
            src_ref=held, dst_ref=held, send_sem=pass_send.at[db, p], recv_sem=pass_recv.at[db, p],
            device_id=ahead(db, 0), device_id_type=MESH,
        )

    def val_copy(db, step):
        to = ahead(db, step)
        at = db * groups + step
        return pltpu.make_async_remote_copy(
            src_ref=prod.at[pl.ds((to["band"] * groups + to["ga"]) * own, own)], dst_ref=land.at[at],
            send_sem=val_send.at[at], recv_sem=val_recv.at[at], device_id=to, device_id_type=MESH,
        )

    def pot_slot(ga):
        step = peer(ga)
        return lax.rem(step, near) * lines + step // near

    def every(act):
        if bands * groups <= 64:
            for step in reversed(range(groups)):
                for db in range(bands):
                    if db or step:
                        act(db, step)
        else:

            def body(at, carry):
                act(at // groups, lax.rem(at, groups))
                return carry

            lax.fori_loop(1, bands * groups, body, 0)

    for z in range(1, lines):
        rot_copy(z, 0).start()
    for p in range(1, near):
        rot_copy(0, p).start()

    small[0].wait()

    def fill_right(step, carry):
        at = pl.multiple_of(step * sz.window, sz.window)
        y_cos = base[0, pl.ds(sz.window + step, 1), :]
        y_sin = base[1, pl.ds(sz.window + step, 1), :]
        z_cos, z_sin = base[0, : sz.window, :], base[1, : sz.window, :]
        cos = split_parts(z_cos * y_cos - z_sin * y_sin)
        sin = split_parts(z_sin * y_cos + z_cos * y_sin)
        for part in range(2):
            right[part, pl.ds(at, sz.window), : sz.wide] = cos[part]
            right[part, pl.ds(at, sz.window), sz.wide :] = sin[part]
            right[part, pl.ds(sz.cols + at, sz.window), : sz.wide] = -sin[part]
            right[part, pl.ds(sz.cols + at, sz.window), sz.wide :] = cos[part]
        return carry

    lax.fori_loop(0, sz.high, fill_right, 0)
    small[1].wait()

    def fill_right_t(step, carry):
        at = pl.multiple_of(step * sz.box, sz.box)
        y_cos = flip[0, pl.ds(sz.box + step, 1), :]
        y_sin = flip[1, pl.ds(sz.box + step, 1), :]
        z_cos, z_sin = flip[0, : sz.box, :], flip[1, : sz.box, :]
        cos = split_parts(z_cos * y_cos - z_sin * y_sin)
        sin = split_parts(z_sin * y_cos + z_cos * y_sin)
        for part in range(2):
            right_t[part, pl.ds(at, sz.box), : sz.cols] = cos[part]
            right_t[part, pl.ds(at, sz.box), sz.cols :] = -sin[part]
            right_t[part, pl.ds(sz.wide + at, sz.box), : sz.cols] = sin[part]
            right_t[part, pl.ds(sz.wide + at, sz.box), sz.cols :] = cos[part]
        return carry

    lax.fori_loop(0, sz.span, fill_right_t, 0)
    for z in range(1, lines):
        rot_copy(z, 0).wait_recv()
        for p in range(1, near):
            rot_copy(z, p).start()
    for z in range(1, lines):
        pot_line(z).start()
    small[2].wait()
    small[3].wait()
    bits = sz.box.bit_length() - 1

    def fill_hot(step, carry):
        at = pl.ds(pl.multiple_of(step * slots, slots), slots)
        cell = idx[:, at]
        n_x = (jnp.right_shift(cell, 2 * bits) + sz.half) & (sz.box - 1)
        n_y = (jnp.right_shift(cell, bits) + sz.half) & (sz.box - 1)
        n_z = (cell + sz.half) & (sz.box - 1)
        live = lax.broadcasted_iota(I32, (1, slots), 1) < cnt[step]
        live = live & (n_x < sz.window) & (n_y < sz.window) & (n_z < sz.window)
        y_high, y_low = n_y // sz.low, n_y % sz.low
        block, fine = y_high // (sz.high // sz.fold), y_high % (sz.high // sz.fold)
        row = jnp.where(live, block * sz.rows + y_low * sz.window + n_x, -1)
        col = fine * sz.window + n_z
        row_at = lax.broadcasted_iota(I32, (sz.fold * sz.rows, slots), 0)
        col_at = lax.broadcasted_iota(I32, (sz.lanes, slots), 0)
        rows_hot[:, at] = jnp.where(row_at == row, 1.0, 0.0).astype(BF16)
        cols_hot[:, at] = jnp.where(col_at == col, 1.0, 0.0).astype(BF16)
        return carry

    lax.fori_loop(0, groups, fill_hot, 0)
    row_at = lax.broadcasted_iota(I32, (sz.rows, sz.cols), 0)
    col_at = lax.broadcasted_iota(I32, (sz.rows, sz.cols), 1)
    n_x = (row_at % sz.window - sz.half).astype(F32)
    n_y = (col_at // sz.window * sz.low + row_at // sz.window - sz.half).astype(F32)
    n_z = (col_at % sz.window - sz.half).astype(F32)
    kin[...] = (8.0 / (sz.box * sz.box)) * (n_x * n_x + n_y * n_y + n_z * n_z)

    slab = 128
    for c in range(2):
        coef_load[c].wait()

        def fill_parts(step, carry, c=c):
            at = pl.multiple_of(step * slab, slab)
            high, low = split_parts(coef[c, pl.ds(at, slab), :])
            parts[0, pl.ds(c * depth + at, slab), :] = high
            parts[1, pl.ds(c * depth + at, slab), :] = low
            return carry

        lax.fori_loop(0, depth // slab, fill_parts, 0)
    for item in small[4:]:
        item.wait()

    rot_self.wait()
    for z in range(lines):
        for p in range(1, near):
            rot_copy(z, p).wait_recv()
    real = rots[:, 0].reshape(panel, depth)
    imag = rots[:, 1].reshape(panel, depth)
    mixer = jnp.concatenate(
        [jnp.concatenate([real, -imag], axis=1), jnp.concatenate([imag, real], axis=1)], axis=0
    )
    high, low = split_parts(mixer)
    first = dot(jnp.concatenate([high, low], axis=0), parts[0])
    mixed = first[: 2 * panel] + first[2 * panel :] + dot(high, parts[1])
    prod[:, 0, :] = mixed[:panel]
    prod[:, 1, :] = mixed[panel:]

    every(lambda db, step: val_copy(db, step).start())
    land[0] = prod[pl.ds(flat * own, own)]
    pot_self.wait()
    for z in range(1, lines):
        pot_line(z).wait_recv()
    for p in reversed(range(1, near)):
        pot_plane(p).start()
    for db in range(1, bands):
        pass_copy(0, db, band).start()

    def relay(pieces):
        for p in pieces:
            pot_plane(p).wait_recv()
            for db in range(1, bands):
                pass_copy(p, db, band).start()

    for i in range(own):

        def scatter(z, carry, i=i):
            total = None
            for p in range(near):
                step = near * z + p
                values = None
                for db in range(bands):
                    if i == 0:
                        if db or p:
                            val_copy(db, step).wait_recv()
                        else:
                            pl.when(z > 0)(lambda: val_copy(0, step).wait_recv())
                    piece = land[db * groups + step, i]
                    values = piece if values is None else values + piece
                at = pl.ds(pl.multiple_of(peer(step) * slots, slots), slots)
                hits = cols_hot[:, at]
                placed = jnp.concatenate(
                    [hits * part[c : c + 1, :] for part in split_parts(values) for c in range(2)], axis=0
                )
                term = dot(rows_hot[:, at], placed, ((1,), (1,)))
                total = term if total is None else total + term
            grid[...] += total
            return carry

        grid[...] = jnp.zeros_like(grid)
        lax.fori_loop(0, lines, scatter, 0)
        if i == 0:
            relay(range(1, near))

        def pot_ready():
            every(lambda db, step: val_copy(db, step).wait_send())
            for z in range(lines):
                for p in range(near):
                    if z or p:
                        rot_copy(z, p).wait_send()
            for z in range(1, lines):
                pot_line(z).wait_send()
            for p in range(1, near):
                pot_plane(p).wait_send()
            for p in range(near):
                for db in range(1, bands):
                    pass_copy(p, db, lax.rem(band + bands - db, bands)).wait_recv()

        apply_kernel(
            sz, i, pot_ready if i == 0 else None, grid, lambda ga: pot[pot_slot(ga)], pot.shape[2], groups, right,
            right_t, fore, back, twist, kin, space, out_ref
        )
    for p in range(near):
        for db in range(1, bands):
            pass_copy(p, db, band).wait_send()


def quarter(real, imag, sign):
    even_r, even_i = real[0] + real[2], imag[0] + imag[2]
    odd_r, odd_i = real[0] - real[2], imag[0] - imag[2]
    both_r, both_i = real[1] + real[3], imag[1] + imag[3]
    gap_r, gap_i = sign * (real[1] - real[3]), sign * (imag[1] - imag[3])
    return (
        (even_r + both_r, even_i + both_i),
        (odd_r - gap_i, odd_i + gap_r),
        (even_r - both_r, even_i - both_i),
        (odd_r + gap_i, odd_i - gap_r),
    )


def apply_kernel(
    sz, index, pot_ready, grid, pot_block, each, groups, right, right_t, fore, back, twist, kin, space, out_ref
):
    whole = 2 * sz.lanes
    summed = grid[:, :whole] + grid[:, whole:]
    field = jnp.concatenate(
        [
            summed[f * sz.rows : (f + 1) * sz.rows, c * sz.lanes : (c + 1) * sz.lanes]
            for c in range(2)
            for f in range(sz.fold)
        ],
        axis=1,
    )
    field_high, field_low = split_parts(field)
    step = 256
    for at in range(0, sz.wide, step):
        halves = []
        for c in range(2):
            here = slice(c * sz.wide + at, c * sz.wide + at + step)
            halves.append(
                dot(field_high, right[0, :, here])
                + (dot(field_low, right[0, :, here]) + dot(field_high, right[1, :, here]))
            )
        real, imag = [], []
        for l in range(sz.low):
            cos, sin = twist[0, l : l + 1, at : at + step], twist[1, l : l + 1, at : at + step]
            a, b = [half[l * sz.window : (l + 1) * sz.window] for half in halves]
            real.append(a * cos - b * sin)
            imag.append(a * sin + b * cos)
        for k, (a, b) in enumerate(quarter(real, imag, 1)):
            high, low = split_parts(jnp.concatenate([a, b], axis=0))
            stacked = jnp.concatenate([high, low, high], axis=0)
            space[k * 2 * sz.box : (k + 1) * 2 * sz.box, at : at + step] = dot(fore[...], stacked)
    if pot_ready is not None:
        pot_ready()
    per = groups // sz.low
    applied = None
    for at in range(0, sz.wide, step):
        real, imag = [], []
        for k in range(sz.low):
            lane = [pot_block(k * per + q) for q in range(at // each, (at + step + each - 1) // each)]
            local = lane[0] if len(lane) == 1 else jnp.concatenate(lane, axis=1)
            here = space[k * 2 * sz.box : (k + 1) * 2 * sz.box, at : at + step]
            high, low = split_parts(here * jnp.concatenate([local, local], axis=0))
            spread = dot(back[...], jnp.concatenate([high, low, high], axis=0))
            real.append(spread[: sz.window])
            imag.append(spread[sz.window :])
        turned = [[], []]
        for l, (a, b) in enumerate(quarter(real, imag, -1)):
            cos, sin = twist[0, l : l + 1, at : at + step], twist[1, l : l + 1, at : at + step]
            turned[0].append(a * cos + b * sin)
            turned[1].append(b * cos - a * sin)
        turned = [jnp.concatenate(rows, axis=0) for rows in turned]
        for c in range(2):
            here = slice(c * sz.wide + at, c * sz.wide + at + step)
            high, low = split_parts(turned[c])
            term = dot(high, right_t[0, here, :]) + (
                dot(low, right_t[0, here, :]) + dot(high, right_t[1, here, :])
            )
            applied = term if applied is None else applied + term
    applied = applied + jnp.concatenate([kin[...], kin[...]], axis=1) * field
    for c in range(2):
        pieces = [
            applied[lo * sz.window : (lo + 1) * sz.window, c * sz.cols + hi * sz.window : c * sz.cols + (hi + 1) * sz.window]
            for hi in range(sz.high)
            for lo in range(sz.low)
        ]
        out_ref[index, c] = jnp.concatenate(pieces, axis=1)


def run(coefficients, rotation, potential, index_map, counts, box):
    bands, groups = lax.axis_size("band"), lax.axis_size("ga")
    sz = Sizes(box, box // 2)
    depth, _, slots = coefficients.shape
    cols = rotation.shape[2]
    panel = cols * groups
    own = panel // (bands * groups)
    consts = [jnp.asarray(t) for t in tables(sz)]
    hbm = pl.BlockSpec(memory_space=pl.ANY)
    dma = pltpu.SemaphoreType.DMA
    return pl.pallas_call(
        functools.partial(whole_kernel, bands, groups, sz),
        out_shape=pltpu.VMEM((own, 2, sz.window, sz.window * sz.window), F32),
        in_specs=[hbm] * 10,
        out_specs=pl.BlockSpec(memory_space=pltpu.VMEM),
        scratch_shapes=[
            pltpu.VMEM((2, depth, slots), F32),
            pltpu.VMEM((2, cols, depth), F32),
            pltpu.VMEM((1, index_map.shape[0]), I32),
            pltpu.SMEM(counts.shape, I32),
            *[pltpu.VMEM(table.shape, table.dtype) for table in consts],
            pltpu.VMEM((2, 2 * sz.cols, 2 * sz.wide), BF16),
            pltpu.VMEM((2, 2 * sz.wide, 2 * sz.cols), BF16),
            pltpu.VMEM((sz.fold * sz.rows, index_map.shape[0]), BF16),
            pltpu.VMEM((sz.lanes, index_map.shape[0]), BF16),
            pltpu.VMEM((2, 2 * depth, slots), BF16),
            pltpu.VMEM((groups, 2, cols, depth), F32),
            pltpu.VMEM((panel, 2, slots), F32),
            pltpu.VMEM((bands * groups, own, 2, slots), F32),
            pltpu.VMEM((groups,) + potential.shape, F32),
            pltpu.VMEM((sz.fold * sz.rows, 4 * sz.lanes), F32),
            pltpu.VMEM((2 * sz.deep, sz.wide), F32),
            pltpu.VMEM((sz.rows, sz.cols), F32),
            dma((10,)),
            dma((2,)),
            dma((groups,)),
            dma((groups,)),
            dma((groups,)),
            dma((groups,)),
            dma((bands, 4)),
            dma((bands, 4)),
            dma((bands * groups,)),
            dma((bands * groups,)),
        ],
        compiler_params=pltpu.CompilerParams(
            collective_id=0, has_side_effects=True, vmem_limit_bytes=60 * 1024 * 1024
        ),
    )(coefficients, rotation.transpose(0, 2, 1), potential, index_map[None], counts, *consts)


def per_device(coefficients, rotation, potential, index_map, counts):
    return run(coefficients, rotation, potential, index_map, counts, potential.shape[0])


def solution(mesh):
    placed = (P("band", None, "ga"), P(None, "band", "ga"), P(None, "ga"), P(), P())
    return jax.shard_map(
        per_device,
        mesh=mesh,
        in_specs=placed,
        out_specs=P(("band", "ga"), None, None, None),
        check_vma=False,
    )
```
